32 devices in a mesh: tp: 4 (over z), cp: 2 (over y), dp: 4 (over x, core).
Axes of the slice: x: 2, y: 2, z: 4, core: 2. Of those that a mesh axis runs over, the one named last changes fastest.
Arguments:
- hidden: bfloat16 [128, 64, 2048], P('dp', 'cp')
- tokens: int32 [128, 64], P('dp', 'cp')
- seq_lens: int32 [128], P('dp')
- norm_gain: float32 [2048], replicated
- w_head: bfloat16 [2048, 49152], P(None, 'tp')
Outputs:
- output 1: float32 [128, 64], P('dp', 'cp')
- output 2: float32 [], replicated
- output 3: bfloat16 [128, 64, 2048], P('dp', 'cp')
- output 4: float32 [2048], replicated
- output 5: float32 [2048, 49152], P(None, 'tp')
All inputs are finite; a program needn't handle non-finite values.
Results may differ from the reference program's by a relative error of at most 0.001.
Values sent between devices are 32-bit elements.
A program may use at most 1 GiB of HBM per device.

```python
import jax
import jax.numpy as jnp
from jax import lax

HIDDEN = 2048
VOCAB_SIZE = 49152
BATCH_ALL = 128
SEQ_LEN = 64
CP_SIZE = 2
ROW_BLOCK = 16
SEG_SIZE = SEQ_LEN // (2 * CP_SIZE)
NORM_EPS = 1e-5


def setup_inputs(seed: int = 0) -> dict:
    key = jax.random.key(seed)
    k_hid, k_tok, k_len, k_gain, k_head = jax.random.split(key, 5)
    hidden = jax.random.normal(k_hid, (BATCH_ALL, SEQ_LEN, HIDDEN), jnp.float32).astype(jnp.bfloat16)
    tokens = jax.random.randint(k_tok, (BATCH_ALL, SEQ_LEN), 0, VOCAB_SIZE, jnp.int32)
    seq_lens = jax.random.randint(k_len, (BATCH_ALL,), SEQ_LEN // 2, SEQ_LEN + 1, jnp.int32).at[0].set(SEQ_LEN)
    norm_gain = 1.0 + 0.3 * jax.random.normal(k_gain, (HIDDEN,), jnp.float32)
    w_head = (2.0 * HIDDEN ** -0.5 * jax.random.normal(k_head, (HIDDEN, VOCAB_SIZE), jnp.float32)).astype(jnp.bfloat16)
    return {'hidden': hidden, 'tokens': tokens, 'seq_lens': seq_lens, 'norm_gain': norm_gain, 'w_head': w_head}


def layout_labels(tokens):
    n_seqs = tokens.shape[0]
    seg_grid = tokens.reshape(n_seqs, CP_SIZE, 2, SEG_SIZE)
    first_end = jnp.concatenate([seg_grid[:, 1:, 0, 0], seg_grid[:, CP_SIZE - 1:, 1, 0]], axis=1)
    second_end = jnp.concatenate([seg_grid[:, :1, 1, 0], seg_grid[:, :CP_SIZE - 1, 1, 0]], axis=1)
    ends = jnp.stack([first_end, second_end], axis=2)
    labels = jnp.concatenate([seg_grid[..., 1:], ends[..., None]], axis=3)
    return labels.reshape(n_seqs, SEQ_LEN)


def layout_positions():
    rank_ids = jnp.arange(CP_SIZE)
    seg_ids = jnp.stack([rank_ids, 2 * CP_SIZE - 1 - rank_ids], axis=1)
    return (seg_ids[:, :, None] * SEG_SIZE + jnp.arange(SEG_SIZE)).reshape(SEQ_LEN)


def reference(hidden, tokens, seq_lens, norm_gain, w_head):
    labels = layout_labels(tokens)
    positions = layout_positions()
    valid_mask = (positions[None, :] + 1 < seq_lens[:, None]).astype(jnp.float32)
    valid_count = jnp.sum(seq_lens - 1).astype(jnp.float32)
    n_blocks = BATCH_ALL * SEQ_LEN // ROW_BLOCK
    rows_h = hidden.reshape(n_blocks, ROW_BLOCK, HIDDEN)
    rows_lab = labels.reshape(n_blocks, ROW_BLOCK)
    rows_valid = valid_mask.reshape(n_blocks, ROW_BLOCK)
    vocab_ids = jnp.arange(VOCAB_SIZE)

    def block_step(acc_pair, block_in):
        dw_acc, dg_acc = acc_pair
        h_rows, lab_rows, valid_rows = block_in
        h_f32 = h_rows.astype(jnp.float32)
        inv_rms = lax.rsqrt(jnp.mean(h_f32 * h_f32, axis=-1, keepdims=True) + NORM_EPS)
        x_hat = h_f32 * inv_rms
        x_norm = (x_hat * norm_gain).astype(jnp.bfloat16)
        logits = jnp.dot(x_norm, w_head, preferred_element_type=jnp.float32)
        row_max = jnp.max(logits, axis=-1, keepdims=True)
        exp_shift = jnp.exp(logits - row_max)
        sum_exp = jnp.sum(exp_shift, axis=-1, keepdims=True)
        log_norm = (row_max + jnp.log(sum_exp))[:, 0]
        onehot = (vocab_ids[None, :] == lab_rows[:, None]).astype(jnp.float32)
        target_logit = jnp.sum(onehot * logits, axis=-1)
        loss_rows = (log_norm - target_logit) * valid_rows
        d_logits = ((exp_shift / sum_exp - onehot) * (valid_rows / valid_count)[:, None]).astype(jnp.bfloat16)
        dx_norm = jnp.dot(d_logits, w_head.T, preferred_element_type=jnp.float32)
        dw_acc = dw_acc + jnp.dot(x_norm.T, d_logits, preferred_element_type=jnp.float32)
        dg_acc = dg_acc + jnp.sum(dx_norm * x_hat, axis=0)
        dx_hat = dx_norm * norm_gain
        d_rows = (inv_rms * (dx_hat - x_hat * jnp.mean(dx_hat * x_hat, axis=-1, keepdims=True))).astype(jnp.bfloat16)
        return (dw_acc, dg_acc), (loss_rows, d_rows)

    init_acc = (jnp.zeros((HIDDEN, VOCAB_SIZE), jnp.float32), jnp.zeros((HIDDEN,), jnp.float32))
    (d_head, d_gain), (loss_blocks, d_blocks) = lax.scan(block_step, init_acc, (rows_h, rows_lab, rows_valid))
    tok_loss = loss_blocks.reshape(BATCH_ALL, SEQ_LEN)
    loss_mean = jnp.sum(tok_loss) / valid_count
    d_hidden = d_blocks.reshape(BATCH_ALL, SEQ_LEN, HIDDEN)
    return tok_loss, loss_mean, d_hidden, d_gain, d_head
```

```python
import jax
import jax.numpy as jnp
from jax import lax
from jax.sharding import PartitionSpec as P
from jax.experimental import pallas as pl
from jax.experimental.pallas import tpu as pltpu

NORM_EPS = 1e-5
F32, BF16 = jnp.float32, jnp.bfloat16
N_COL = 8
TOK = 1024
VMEM = 64_000_000


def _params(**kw):
    return pltpu.CompilerParams(vmem_limit_bytes=VMEM, **kw)


def _cost(flops, bytes_accessed):
    return pl.CostEstimate(flops=int(flops), bytes_accessed=int(bytes_accessed), transcendentals=0)


def _norm(hidden, gain):
    rows, width = hidden.shape
    step = 256

    def kernel(h_ref, g_ref, x_ref, xs_ref):
        h = h_ref[...].astype(F32)
        inv_rms = lax.rsqrt(jnp.mean(h * h, axis=-1, keepdims=True) + NORM_EPS)
        x = (h * inv_rms * g_ref[...]).astype(BF16)
        x_ref[...] = x
        xs_ref[...] = x.astype(F32)

    return pl.pallas_call(
        kernel,
        grid=(rows // step,),
        out_shape=[jax.ShapeDtypeStruct((rows, width), BF16), jax.ShapeDtypeStruct((rows, width), F32)],
        in_specs=[pl.BlockSpec((step, width), lambda i: (i, 0)), pl.BlockSpec((1, width), lambda i: (0, 0))],
        out_specs=[pl.BlockSpec((step, width), lambda i: (i, 0)), pl.BlockSpec((step, width), lambda i: (i, 0))],
        compiler_params=_params(),
        cost_estimate=_cost(rows * width * 256, rows * width * 8),
    )(hidden, gain)


def _logits(x, labels, w):
    rows, width = x.shape
    vocab = w.shape[1]
    cols = 1024
    steps = vocab // cols

    def kernel(x_ref, lab_ref, w_ref, z_ref, st_ref, m_ref, s_ref, t_ref):
        i = pl.program_id(0)

        @pl.when(i == 0)
        def _():
            m_ref[...] = jnp.full_like(m_ref, -jnp.inf)
            s_ref[...] = jnp.zeros_like(s_ref)
            t_ref[...] = jnp.zeros_like(t_ref)

        z = jnp.dot(x_ref[...], w_ref[...], preferred_element_type=F32)
        z_ref[...] = z
        rel = lab_ref[...] - cols * i
        lane = lax.broadcasted_iota(jnp.int32, (rows, 128), 1)
        old = m_ref[...]
        top = old
        for g in range(cols // 128):
            top = jnp.maximum(top, z[:, g * 128:(g + 1) * 128])
        total = s_ref[...] * jnp.exp(old - top)
        target = t_ref[...]
        for g in range(cols // 128):
            z_g = z[:, g * 128:(g + 1) * 128]
            total = total + jnp.exp(z_g - top)
            target = target + jnp.where(lane == rel - g * 128, z_g, 0.0)
        m_ref[...] = top
        s_ref[...] = total
        t_ref[...] = target

        @pl.when(i == steps - 1)
        def _():
            row_max = jnp.max(top, axis=1, keepdims=True)
            row_sum = jnp.sum(total * jnp.exp(top - row_max), axis=1, keepdims=True)
            row_target = jnp.sum(target, axis=1, keepdims=True)
            st_ref[...] = jnp.where(lane == 0, row_max, jnp.where(lane == 1, row_sum, row_target))

    return pl.pallas_call(
        kernel,
        grid=(steps,),
        out_shape=[jax.ShapeDtypeStruct((rows, vocab), F32), jax.ShapeDtypeStruct((rows, 128), F32)],
        in_specs=[pl.BlockSpec((rows, width), lambda i: (0, 0)), pl.BlockSpec((rows, 1), lambda i: (0, 0)), pl.BlockSpec((width, cols), lambda i: (0, i))],
        out_specs=[pl.BlockSpec((rows, cols), lambda i: (0, i)), pl.BlockSpec((rows, 128), lambda i: (0, 0))],
        scratch_shapes=[pltpu.VMEM((rows, 128), F32)] * 3,
        compiler_params=_params(),
        cost_estimate=_cost(2 * rows * width * vocab, vocab * (2 * width + 4 * rows)),
    )(x, labels, w)


def _d_logits(z, meta, first):
    rel = meta[:, 1:2].astype(jnp.int32) - first
    hit = lax.broadcasted_iota(jnp.int32, z.shape, 1) == rel
    return ((jnp.exp(z - meta[:, 0:1]) - jnp.where(hit, 1.0, 0.0)) * meta[:, 2:3]).astype(BF16)


def _d_norm(z, meta, w):
    rows, vocab = z.shape
    width = w.shape[0]
    cols = 1024

    def kernel(z_ref, meta_ref, w_ref, acc_ref):
        i = pl.program_id(0)

        @pl.when(i == 0)
        def _():
            acc_ref[...] = jnp.zeros_like(acc_ref)

        d = _d_logits(z_ref[...], meta_ref[...], lax.axis_index('tp') * vocab + i * cols)
        acc_ref[...] += lax.dot_general(d, w_ref[...], (((1,), (1,)), ((), ())), preferred_element_type=F32)

    return pl.pallas_call(
        kernel,
        grid=(vocab // cols,),
        out_shape=jax.ShapeDtypeStruct((rows, width), F32),
        in_specs=[pl.BlockSpec((rows, cols), lambda i: (0, i)), pl.BlockSpec((rows, 4), lambda i: (0, 0)), pl.BlockSpec((width, cols), lambda i: (0, i))],
        out_specs=pl.BlockSpec((rows, width), lambda i: (0, 0)),
        compiler_params=_params(),
        cost_estimate=_cost(2 * rows * width * vocab, vocab * (2 * width + 4 * rows)),
    )(z, meta, w)


def _d_head_first(x, meta, w, cols):
    rows, width = x.shape
    vocab = w.shape[1]
    half = vocab // 2

    def kernel(x_ref, meta_ref, w_ref, acc_ref):
        first = lax.axis_index('tp') * vocab + lax.axis_index('dp') % 2 * half + pl.program_id(0) * cols

        @pl.when(pl.program_id(1) == 0)
        def _():
            acc_ref[...] = jnp.zeros_like(acc_ref)

        x_b = x_ref[...].astype(BF16)
        d = _d_logits(jnp.dot(x_b, w_ref[...], preferred_element_type=F32), meta_ref[...], first)
        acc_ref[...] += lax.dot_general(x_b, d, (((0,), (0,)), ((), ())), preferred_element_type=F32)

    return pl.pallas_call(
        kernel,
        grid=(half // cols, rows // TOK),
        out_shape=jax.ShapeDtypeStruct((width, half), F32),
        in_specs=[
            pl.BlockSpec((TOK, width), lambda j, i: (i, 0)),
            pl.BlockSpec((TOK, 4), lambda j, i: (i, 0)),
            pl.BlockSpec((width, cols), lambda j, i: (0, lax.axis_index('dp') % 2 * (half // cols) + j)),
        ],
        out_specs=pl.BlockSpec((width, cols), lambda j, i: (0, j)),
        compiler_params=_params(),
        cost_estimate=_cost(4 * rows * width * half, half // cols * rows * width * 4),
    )(x, meta, w)


def _d_head_last(x, meta, w, first_part, cols):
    rows, width = x.shape
    vocab = w.shape[1]
    half = vocab // 2
    n_col = half // cols
    n_tok = rows // TOK

    def kernel(x_ref, meta_ref, w_ref, init_ref, out_ref, acc_ref, init_sem, own_sem, send_sem, recv_sem):
        j, i = pl.program_id(0), pl.program_id(1)
        me = lax.axis_index('dp')
        core = me % 2
        peer = me + 1 - 2 * core
        slot = j % 2

        def own(jj):
            at = pl.ds(pl.multiple_of(core * half + jj * cols, 128), cols)
            return pltpu.make_async_copy(acc_ref.at[jj % 2], out_ref.at[:, at], own_sem.at[jj % 2])

        def send(jj):
            at = pl.ds(pl.multiple_of(core * half + jj * cols, 128), cols)
            return pltpu.make_async_remote_copy(acc_ref.at[jj % 2], out_ref.at[:, at], send_sem.at[jj % 2], recv_sem.at[jj], device_id={'dp': peer}, device_id_type=pl.DeviceIdType.MESH)

        def arrival(jj):
            at = pl.ds(pl.multiple_of((1 - core) * half + jj * cols, 128), cols)
            return pltpu.make_async_remote_copy(acc_ref.at[jj % 2], out_ref.at[:, at], send_sem.at[jj % 2], recv_sem.at[jj], device_id={'dp': peer}, device_id_type=pl.DeviceIdType.MESH)

        def init(jj):
            return pltpu.make_async_copy(init_ref.at[:, pl.ds(pl.multiple_of(jj * cols, 128), cols)], acc_ref.at[jj % 2], init_sem.at[jj % 2])

        @pl.when((j == 0) & (i == 0))
        def _():
            init(0).start()
            barrier = pltpu.get_barrier_semaphore()
            pl.semaphore_signal(barrier, inc=1, device_id={'dp': peer}, device_id_type=pl.DeviceIdType.MESH)
            pl.semaphore_wait(barrier, 1)

        @pl.when(i == 0)
        def _():
            init(j).wait()

        @pl.when(i == n_tok // 2)
        def _():
            @pl.when(j >= 1)
            def _():
                own(j - 1).wait()
                send(j - 1).wait_send()

            @pl.when(j < n_col - 1)
            def _():
                init(j + 1).start()

        first = lax.axis_index('tp') * vocab + core * half + j * cols
        x_b = x_ref[...].astype(BF16)
        d = _d_logits(jnp.dot(x_b, w_ref[...], preferred_element_type=F32), meta_ref[...], first)
        acc_ref[slot] += lax.dot_general(x_b, d, (((0,), (0,)), ((), ())), preferred_element_type=F32)

        @pl.when(i == n_tok - 1)
        def _():
            own(j).start()
            send(j).start()

        @pl.when((j == n_col - 1) & (i == n_tok - 1))
        def _():
            own(j).wait()
            send(j).wait_send()
            for jj in range(n_col):
                arrival(jj).wait_recv()

    return pl.pallas_call(
        kernel,
        grid=(n_col, n_tok),
        out_shape=jax.ShapeDtypeStruct((width, vocab), F32),
        in_specs=[
            pl.BlockSpec((TOK, width), lambda j, i: (i, 0)),
            pl.BlockSpec((TOK, 4), lambda j, i: (i, 0)),
            pl.BlockSpec((width, cols), lambda j, i: (0, lax.axis_index('dp') % 2 * n_col + j)),
            pl.BlockSpec(memory_space=pl.ANY),
        ],
        out_specs=pl.BlockSpec(memory_space=pl.ANY),
        scratch_shapes=[pltpu.VMEM((2, width, cols), F32)] + [pltpu.SemaphoreType.DMA((2,))] * 3 + [pltpu.SemaphoreType.DMA((n_col,))],
        compiler_params=_params(collective_id=0, has_side_effects=True),
        cost_estimate=_cost(4 * rows * width * half, half // cols * rows * width * 4),
    )(x, meta, w, first_part)


def _finish(hidden, d_x_norm, gain):
    rows, width = hidden.shape
    step = 256

    def kernel(h_ref, d_ref, g_ref, dh_ref, dg_ref):
        @pl.when(pl.program_id(0) == 0)
        def _():
            dg_ref[...] = jnp.zeros_like(dg_ref)

        h = h_ref[...].astype(F32)
        inv_rms = lax.rsqrt(jnp.mean(h * h, axis=-1, keepdims=True) + NORM_EPS)
        x = h * inv_rms
        d = d_ref[...]
        dg_ref[...] += jnp.sum(d * x, axis=0, keepdims=True)
        d_x = d * g_ref[...]
        dh_ref[...] = (inv_rms * (d_x - x * jnp.mean(d_x * x, axis=-1, keepdims=True))).astype(BF16)

    return pl.pallas_call(
        kernel,
        grid=(rows // step,),
        out_shape=[jax.ShapeDtypeStruct((rows, width), BF16), jax.ShapeDtypeStruct((1, width), F32)],
        in_specs=[pl.BlockSpec((step, width), lambda i: (i, 0)), pl.BlockSpec((step, width), lambda i: (i, 0)), pl.BlockSpec((1, width), lambda i: (0, 0))],
        out_specs=[pl.BlockSpec((step, width), lambda i: (i, 0)), pl.BlockSpec((1, width), lambda i: (0, 0))],
        compiler_params=_params(),
        cost_estimate=_cost(rows * width * 256, rows * width * 8),
    )(hidden, d_x_norm, gain)


def solution(mesh):
    n_tp, n_cp, n_dp = mesh.shape['tp'], mesh.shape['cp'], mesh.shape['dp']
    groups = n_cp * n_dp

    def part_fn(hidden, tokens, seq_lens, norm_gain, w_head):
        n_seq, local_len, width = hidden.shape
        n_tok = n_seq * local_len
        half_tok = n_tok // 2
        sub = half_tok // n_tp
        seg_len = local_len // 2
        vocab_local = w_head.shape[1]
        cp_rank = lax.axis_index('cp')
        tp_rank = lax.axis_index('tp')
        me = cp_rank * n_dp + lax.axis_index('dp')
        gain = norm_gain.reshape(1, width)
        hidden_rows = hidden.reshape(n_tok, width)

        x_norm, x_send = _norm(hidden_rows, gain)
        x_a = lax.all_gather(x_send[:half_tok], ('cp', 'dp'), axis=0, tiled=True)
        x_b = lax.all_gather(lax.dynamic_slice_in_dim(x_send, half_tok + tp_rank * sub, sub), ('tp', 'cp', 'dp'), axis=0, tiled=True)

        edge = lax.ppermute(jnp.where(cp_rank == 0, tokens[:, seg_len], tokens[:, 0]), 'cp', [(0, 1), (1, 0)])
        first_end = jnp.where(cp_rank == 0, edge, tokens[:, seg_len])
        second_end = jnp.where(cp_rank == 0, 0, edge)
        labels = jnp.concatenate([tokens[:, 1:seg_len], first_end[:, None], tokens[:, seg_len + 1:], second_end[:, None]], axis=1)
        seg_pos = jnp.arange(seg_len)
        positions = jnp.concatenate([cp_rank * seg_len + seg_pos, (2 * n_cp - 1 - cp_rank) * seg_len + seg_pos])
        valid = (positions[None, :] + 1 < seq_lens[:, None]).astype(F32).reshape(n_tok)
        labels = labels.reshape(n_tok)

        logits, row_stats = _logits(x_norm, (labels - tp_rank * vocab_local).reshape(n_tok, 1), w_head)

        mine = jnp.concatenate([row_stats[:, :3].T, labels.astype(F32)[None], valid[None]])
        stats = lax.all_gather(mine, ('tp', 'cp', 'dp'), axis=0, tiled=False).reshape(n_tp, groups, 5, n_tok)
        all_max = jnp.max(stats[:, :, 0], axis=0)
        all_sum = jnp.sum(stats[:, :, 1] * jnp.exp(stats[:, :, 0] - all_max[None]), axis=0)
        all_lse = all_max + jnp.log(all_sum)
        all_valid = stats[0, :, 4]
        all_loss = (all_lse - jnp.sum(stats[:, :, 2], axis=0)) * all_valid
        valid_count = jnp.sum(all_valid)
        loss_mean = jnp.sum(all_loss) / valid_count
        tok_loss = lax.dynamic_index_in_dim(all_loss, me, 0, keepdims=False).reshape(n_seq, local_len)
        meta = jnp.stack([all_lse, stats[0, :, 3], all_valid / valid_count, all_valid], axis=-1)
        meta_own = lax.dynamic_index_in_dim(meta, me, 0, keepdims=False)
        meta_a = meta[:, :half_tok].reshape(groups * half_tok, 4)
        meta_b = meta[:, half_tok:].reshape(groups, n_tp, sub, 4).transpose(1, 0, 2, 3).reshape(groups * half_tok, 4)

        d_x_norm = _d_norm(logits, meta_own, w_head)
        d_x_norm = lax.psum(d_x_norm, 'tp')
        cols = vocab_local // 2 // N_COL
        part_a = _d_head_first(x_a, meta_a, w_head, cols)
        d_head = _d_head_last(x_b, meta_b, w_head, part_a, cols)
        d_hidden, d_gain = _finish(hidden_rows, d_x_norm, gain)
        d_gain = lax.psum(d_gain.reshape(width), ('cp', 'dp'))
        return tok_loss, loss_mean, d_hidden.reshape(hidden.shape), d_gain, d_head

    return jax.shard_map(part_fn, mesh=mesh, in_specs=(P('dp', 'cp', None), P('dp', 'cp'), P('dp'), P(None), P(None, 'tp')), out_specs=(P('dp', 'cp'), P(), P('dp', 'cp', None), P(None), P(None, 'tp')), check_vma=False)
```

```python
import jax
import jax.numpy as jnp
from jax import lax
from jax.sharding import PartitionSpec as P
from jax.experimental import pallas as pl
from jax.experimental.pallas import tpu as pltpu

NORM_EPS = 1e-5
F32, BF16 = jnp.float32, jnp.bfloat16
COLS = 512
TOK = 1024
VMEM = 63_000_000
MESH = pl.DeviceIdType.MESH


def _params(**kw):
    return pltpu.CompilerParams(vmem_limit_bytes=VMEM, **kw)


def _cost(flops, bytes_accessed):
    return pl.CostEstimate(flops=int(flops), bytes_accessed=int(bytes_accessed), transcendentals=0)


def _any():
    return pl.BlockSpec(memory_space=pl.ANY)


def _whole(shape):
    return pl.BlockSpec(shape, lambda *ids: (0,) * len(shape))


def _meet(peers):
    barrier = pltpu.get_barrier_semaphore()
    for peer in peers:
        pl.semaphore_signal(barrier, inc=1, device_id=peer, device_id_type=MESH)
    pl.semaphore_wait(barrier, len(peers))


def _send(src, dst, send_sem, recv_sem, peer):
    return pltpu.make_async_remote_copy(src, dst, send_sem, recv_sem, device_id=peer, device_id_type=MESH)


def _plane(n_dp):
    me = lax.axis_index('cp') * n_dp + lax.axis_index('dp')
    return me, lambda p: {'cp': p // n_dp, 'dp': p % n_dp}


def _columns(rows):
    return jnp.concatenate([rows, jnp.zeros((120, rows.shape[1]), F32)], axis=0).T


def _norm(hidden, gain):
    rows, width = hidden.shape
    step = 128
    n = rows // step

    def kernel(h_ref, g_ref, x_ref, xa_ref, xb_ref):
        i = pl.program_id(0)
        h = h_ref[...].astype(F32)
        inv_rms = lax.rsqrt(jnp.mean(h * h, axis=-1, keepdims=True) + NORM_EPS)
        x = (h * inv_rms * g_ref[...]).astype(BF16)
        x_ref[...] = x

        @pl.when(i < n // 2)
        def _():
            xa_ref[...] = x.astype(F32)

        @pl.when(i >= n // 2)
        def _():
            xb_ref[...] = x.astype(F32)

    half = jax.ShapeDtypeStruct((rows // 2, width), F32)
    return pl.pallas_call(
        kernel,
        grid=(n,),
        out_shape=[jax.ShapeDtypeStruct((rows, width), BF16), half, half],
        in_specs=[pl.BlockSpec((step, width), lambda i: (i, 0)), _whole((1, width))],
        out_specs=[
            pl.BlockSpec((step, width), lambda i: (i, 0)),
            pl.BlockSpec((step, width), lambda i: (jnp.minimum(i, n // 2 - 1), 0)),
            pl.BlockSpec((step, width), lambda i: (jnp.maximum(i - n // 2, 0), 0)),
        ],
        compiler_params=_params(),
        cost_estimate=_cost(rows * width * 256, rows * width * 8),
    )(hidden, gain)


def _logits(x, row, count, w, n_tp, n_dp):
    rows, width = x.shape
    vocab = w.shape[1]
    cols = 1024
    steps = vocab // cols

    def kernel(x_ref, row_ref, cnt_ref, cnt_any, w_ref, z_ref, mrow_ref, mcol_ref, m_ref, s_ref, t_ref, lab_ref, st_buf, cnt_buf, cs_sem, cr_sem, ss_sem, sr_sem):
        i = pl.program_id(0)
        tp, dp = lax.axis_index('tp'), lax.axis_index('dp')

        def tell(k):
            return _send(cnt_any, cnt_buf.at[k - 1], cs_sem.at[k - 1], cr_sem.at[k - 1], {'dp': (dp + k) % n_dp})

        def give(k, slot):
            return _send(st_buf.at[slot], st_buf.at[slot], ss_sem.at[k - 1], sr_sem.at[k - 1], {'tp': (tp + k) % n_tp})

        @pl.when(i == 0)
        def _():
            _meet([{'tp': (tp + k) % n_tp} for k in range(1, n_tp)] + [{'dp': (dp + k) % n_dp} for k in range(1, n_dp)])
            for k in range(1, n_dp):
                tell(k).start()
            m_ref[...] = jnp.full_like(m_ref, -jnp.inf)
            s_ref[...] = jnp.zeros_like(s_ref)
            t_ref[...] = jnp.zeros_like(t_ref)
            lab_ref[...] = _columns(row_ref[...])

        z = jnp.dot(x_ref[...], w_ref[...], preferred_element_type=F32)
        z_ref[...] = z
        rel = lab_ref[:, 0:1].astype(jnp.int32) - (tp * vocab + cols * i)
        lane = lax.broadcasted_iota(jnp.int32, (rows, 128), 1)
        old = m_ref[...]
        top = old
        for g in range(cols // 128):
            top = jnp.maximum(top, z[:, g * 128:(g + 1) * 128])
        total = s_ref[...] * jnp.exp(old - top)
        target = t_ref[...]
        for g in range(cols // 128):
            z_g = z[:, g * 128:(g + 1) * 128]
            total = total + jnp.exp(z_g - top)
            target = target + jnp.where(lane == rel - g * 128, z_g, 0.0)
        m_ref[...] = top
        s_ref[...] = total
        t_ref[...] = target

        @pl.when(i == steps - 1)
        def _():
            top, total = m_ref[...], s_ref[...]
            row_max = jnp.max(top, axis=1, keepdims=True)
            row_sum = jnp.sum(total * jnp.exp(top - row_max), axis=1, keepdims=True)
            row_target = jnp.sum(t_ref[...], axis=1, keepdims=True)
            st_buf[tp] = jnp.where(lane == 0, row_max, jnp.where(lane == 1, row_sum, row_target)).T[0:8]
            for k in range(1, n_dp):
                tell(k).wait()
            for k in range(1, n_tp):
                give(k, tp).start()
            n_valid = cnt_ref[0:1, 0:1]
            for k in range(1, n_dp):
                n_valid = n_valid + cnt_buf[k - 1, 0:1, 0:1]
            for k in range(1, n_tp):
                give(k, tp).wait_send()
                give(k, (tp + n_tp - k) % n_tp).wait_recv()
            top = st_buf[0, 0:1]
            for k in range(1, n_tp):
                top = jnp.maximum(top, st_buf[k, 0:1])
            total = st_buf[0, 1:2] * jnp.exp(st_buf[0, 0:1] - top)
            target = st_buf[0, 2:3]
            for k in range(1, n_tp):
                total = total + st_buf[k, 1:2] * jnp.exp(st_buf[k, 0:1] - top)
                target = target + st_buf[k, 2:3]
            lse = top + jnp.log(total)
            valid = row_ref[1:2]
            sub = lax.broadcasted_iota(jnp.int32, (8, rows), 0)
            meta = jnp.where(sub == 0, lse, jnp.where(sub == 1, row_ref[0:1], jnp.where(sub == 2, valid / n_valid, jnp.where(sub == 3, (lse - target) * valid, n_valid))))
            mrow_ref[...] = meta
            mcol_ref[...] = _columns(meta)

    return pl.pallas_call(
        kernel,
        grid=(steps,),
        out_shape=[jax.ShapeDtypeStruct((rows, vocab), F32), jax.ShapeDtypeStruct((8, rows), F32), jax.ShapeDtypeStruct((rows, 128), F32)],
        in_specs=[_whole((rows, width)), _whole((8, rows)), _whole((8, 128)), _any(), pl.BlockSpec((width, cols), lambda i: (0, i))],
        out_specs=[pl.BlockSpec((rows, cols), lambda i: (0, i)), _whole((8, rows)), _whole((rows, 128))],
        scratch_shapes=[pltpu.VMEM((rows, 128), F32)] * 4
        + [pltpu.VMEM((n_tp, 8, rows), F32), pltpu.VMEM((n_dp - 1, 8, 128), F32)]
        + [pltpu.SemaphoreType.DMA((n_dp - 1,))] * 2 + [pltpu.SemaphoreType.DMA((n_tp - 1,))] * 2,
        compiler_params=_params(collective_id=1, has_side_effects=True),
        cost_estimate=_cost(2 * rows * width * vocab, vocab * (2 * width + 4 * rows)),
    )(x, row, count, count, w)


def _d_logits(z, meta, first):
    rel = meta[:, 1:2].astype(jnp.int32) - first
    hit = lax.broadcasted_iota(jnp.int32, z.shape, 1) == rel
    return ((jnp.exp(z - meta[:, 0:1]) - jnp.where(hit, 1.0, 0.0)) * meta[:, 2:3]).astype(BF16)


def _d_norm(z, mcol, mrow, w, n_cp, n_dp):
    rows, vocab = z.shape
    width = w.shape[0]
    cols = 1024
    steps = vocab // cols
    groups = n_cp * n_dp

    def kernel(z_ref, mcol_ref, mrow_any, w_ref, acc_ref, all_ref, buf, own_sem, send_sem, recv_sem):
        i = pl.program_id(0)
        me, device = _plane(n_dp)
        own = pltpu.make_async_copy(mrow_any, buf.at[me], own_sem)

        def give(e, slot):
            return _send(mrow_any, buf.at[slot], send_sem.at[e - 1], recv_sem.at[e - 1], device((me + e) % groups))

        @pl.when(i == 0)
        def _():
            own.start()
            _meet([device((me + e) % groups) for e in range(1, groups)])
            for e in range(1, groups):
                give(e, me).start()
            acc_ref[...] = jnp.zeros_like(acc_ref)

        d = _d_logits(z_ref[...], mcol_ref[...], lax.axis_index('tp') * vocab + i * cols)
        acc_ref[...] += lax.dot_general(d, w_ref[...], (((1,), (1,)), ((), ())), preferred_element_type=F32)

        @pl.when(i == steps - 1)
        def _():
            own.wait()
            for e in range(1, groups):
                give(e, me).wait_send()
                give(e, (me + groups - e) % groups).wait_recv()
            all_ref[...] = buf[...]

    return pl.pallas_call(
        kernel,
        grid=(steps,),
        out_shape=[jax.ShapeDtypeStruct((rows, width), F32), jax.ShapeDtypeStruct((groups, 8, rows), F32)],
        in_specs=[pl.BlockSpec((rows, cols), lambda i: (0, i)), _whole((rows, 128)), _any(), pl.BlockSpec((width, cols), lambda i: (0, i))],
        out_specs=[_whole((rows, width)), _whole((groups, 8, rows))],
        scratch_shapes=[pltpu.VMEM((groups, 8, rows), F32), pltpu.SemaphoreType.DMA] + [pltpu.SemaphoreType.DMA((groups - 1,))] * 2,
        compiler_params=_params(collective_id=2, has_side_effects=True),
        cost_estimate=_cost(2 * rows * width * vocab, vocab * (2 * width + 4 * rows)),
    )(z, mcol, mrow, w)


class _Split:
    def __init__(self, vocab, groups):
        self.vocab, self.groups = vocab, groups
        self.blocks = vocab // COLS
        self.n_f = (self.blocks - groups - 2) // 2
        self.g0 = 2 * self.n_f
        self.r0 = self.g0 + groups
        self.n = 1 + self.n_f

    def block(self, b, me, core):
        return jnp.where(b == 0, self.g0 + me, core * self.n_f + b - 1)


def _part(x_b, meta, w, first):
    rows = jnp.concatenate([meta[k] for k in range(meta.shape[0])], axis=1) if meta.shape[0] > 1 else meta[0]
    d = _d_logits(jnp.dot(x_b, w, preferred_element_type=F32), _columns(rows), first)
    return lax.dot_general(x_b, d, (((0,), (0,)), ((), ())), preferred_element_type=F32)


def _head_a(x, meta, w, d_x_norm, split, n_tp, n_dp):
    rows, width = x.shape
    half = meta.shape[2] // 2
    n_tok = rows // TOK
    sub = d_x_norm.shape[0] // n_tp

    def kernel(x_ref, meta_ref, w_ref, dx_any, acc_ref, xb_ref, got_any, leg, mid, send_sem, recv_sem, leg_sem, mid_sem):
        b, i = pl.program_id(0), pl.program_id(1)
        tp = lax.axis_index('tp')
        me, _ = _plane(n_dp)
        inner = (tp == 1) | (tp == 2)
        far = jnp.where(tp < 2, 3, 0)

        def quarter(q):
            return dx_any.at[pl.ds(pl.multiple_of(q * sub, 8), sub)]

        def give(to, src):
            return _send(src, got_any.at[tp], send_sem.at[to], recv_sem.at[tp], {'tp': to})

        def arrive(frm):
            return _send(mid, got_any.at[frm], send_sem.at[frm], recv_sem.at[frm], {'tp': frm})

        first_leg = _send(quarter(far), leg, leg_sem.at[0], leg_sem.at[1], {'tp': jnp.where(tp == 0, 1, 2)})
        load_mid = pltpu.make_async_copy(quarter(far), mid, mid_sem)

        @pl.when((b == 0) & (i == 0))
        def _():
            _meet([{'tp': (tp + k) % n_tp} for k in range(1, n_tp)])

            @pl.when(inner)
            def _():
                load_mid.start()
                give(3 - tp, quarter(3 - tp)).start()
                give(3 - far, quarter(3 - far)).start()

            @pl.when(jnp.logical_not(inner))
            def _():
                first_leg.start()
                for gap in (2, 1):
                    to = jnp.where(tp == 0, gap, 3 - gap)
                    give(to, quarter(to)).start()

        @pl.when((b == split.n // 2 - 1) & (i == 0) & inner)
        def _():
            load_mid.wait()
            first_leg.wait_recv()
            mid[...] += leg[...]

        @pl.when((b == split.n // 2 - 1) & (i == 1) & inner)
        def _():
            give(far, mid).start()

        @pl.when(i == 0)
        def _():
            acc_ref[...] = jnp.zeros_like(acc_ref)

        x_b = x_ref[...].astype(BF16)

        @pl.when(b == 0)
        def _():
            xb_ref[...] = x_b

        first = tp * split.vocab + split.block(b, me, lax.axis_index('dp') % 2) * COLS
        acc_ref[...] += _part(x_b, meta_ref, w_ref[...], first)

        @pl.when((b == split.n - 1) & (i == n_tok - 1))
        def _():
            @pl.when(inner)
            def _():
                for q in range(n_tp):
                    @pl.when(tp != q)
                    def _():
                        give(q, mid).wait_send()
                        arrive(q).wait_recv()

            @pl.when(jnp.logical_not(inner))
            def _():
                first_leg.wait_send()
                for q in (1, 2):
                    give(q, mid).wait_send()
                    arrive(q).wait_recv()

    return pl.pallas_call(
        kernel,
        grid=(split.n, n_tok),
        out_shape=[jax.ShapeDtypeStruct((width, split.n * COLS), F32), jax.ShapeDtypeStruct((2 * rows, width), BF16), jax.ShapeDtypeStruct((n_tp, sub, width), F32)],
        in_specs=[
            pl.BlockSpec((TOK, width), lambda b, i: (i, 0)),
            pl.BlockSpec((TOK // half, 8, half), lambda b, i: (i, 0, 0)),
            pl.BlockSpec((width, COLS), lambda b, i: (0, split.block(b, _plane(n_dp)[0], lax.axis_index('dp') % 2))),
            _any(),
        ],
        out_specs=[pl.BlockSpec((width, COLS), lambda b, i: (0, b)), pl.BlockSpec((TOK, width), lambda b, i: (jnp.where(b == 0, i, n_tok - 1), 0)), _any()],
        scratch_shapes=[pltpu.VMEM((sub, width), F32)] * 2 + [pltpu.SemaphoreType.DMA((n_tp,))] * 2 + [pltpu.SemaphoreType.DMA((2,)), pltpu.SemaphoreType.DMA],
        compiler_params=_params(collective_id=3, has_side_effects=True),
        cost_estimate=_cost(4 * rows * width * split.n * COLS, split.n * rows * width * 4),
    )(x, meta, w, d_x_norm)


def _head_g(x, meta, w, part, x_all, split, n_dp):
    rows, width = x.shape
    half = meta.shape[2] // 2
    n_tok = rows // half

    def kernel(x_ref, meta_ref, w_ref, init_ref, _, acc_ref, xb_ref):
        @pl.when(pl.program_id(0) == 0)
        def _():
            acc_ref[...] = init_ref[...]

        x_b = x_ref[...].astype(BF16)
        xb_ref[...] = x_b
        first = lax.axis_index('tp') * split.vocab + (split.g0 + _plane(n_dp)[0]) * COLS
        acc_ref[...] += _part(x_b, meta_ref, w_ref[...], first)

    return pl.pallas_call(
        kernel,
        grid=(n_tok,),
        out_shape=[jax.ShapeDtypeStruct((width, COLS), F32), jax.ShapeDtypeStruct((2 * rows, width), BF16)],
        in_specs=[
            pl.BlockSpec((half, width), lambda i: (i, 0)),
            pl.BlockSpec((1, 8, half), lambda i: (i, 0, 1)),
            pl.BlockSpec((width, COLS), lambda i: (0, split.g0 + _plane(n_dp)[0])),
            _whole((width, COLS)),
            _any(),
        ],
        out_specs=[_whole((width, COLS)), pl.BlockSpec((half, width), lambda i: (n_tok + i, 0))],
        input_output_aliases={4: 1},
        compiler_params=_params(),
        cost_estimate=_cost(4 * rows * width * COLS, rows * width * 6),
    )(x, meta, w, part, x_all)


def _head_f(x, meta, w, part, d_hid, d_gain, split, n_tp, n_cp, n_dp):
    width = x.shape[1]
    rows = x.shape[0] // 2
    half = meta.shape[2] // 2
    n_f, groups = split.n_f, n_cp * n_dp
    n_tok = rows // TOK
    sub = d_hid.shape[0]

    def kernel(x_ref, meta_ref, w_ref, init_any, dh_any, dg_any, out_any, dhall_any, dg_ref, acc, dg_z, dg_s, dg_x, init_sem, own_sem, send_sem, recv_sem, hs_sem, hr_sem, fs_sem, zs_sem, zr_sem, zo_sem, xs_sem, xr_sem):
        j, i = pl.program_id(0), pl.program_id(1)
        tp, dp = lax.axis_index('tp'), lax.axis_index('dp')
        me, device = _plane(n_dp)
        core = dp % 2
        slot = j % 2
        z_peers = [{'tp': (tp + k) % n_tp} for k in range(1, n_tp)]

        def at(owner, jj):
            return out_any.at[:, pl.ds(pl.multiple_of((owner * n_f + jj) * COLS, COLS), COLS)]

        def init(jj):
            return pltpu.make_async_copy(init_any.at[:, pl.ds(pl.multiple_of((jj + 1) * COLS, COLS), COLS)], acc.at[jj % 2], init_sem.at[jj % 2])

        def own(jj):
            return pltpu.make_async_copy(acc.at[jj % 2], at(core, jj), own_sem.at[jj % 2])

        def swap(jj, owner):
            return _send(acc.at[jj % 2], at(owner, jj), send_sem.at[jj % 2], recv_sem.at[jj], {'dp': dp + 1 - 2 * core})

        def hid(to):
            return _send(dh_any, dhall_any.at[tp], hs_sem.at[to], hr_sem.at[tp], {'tp': to})

        def relay(row, to):
            return _send(dhall_any.at[row], dhall_any.at[row], fs_sem, hr_sem.at[row], {'tp': to})

        def gain_z(k, row):
            return _send(dg_any, dg_z.at[row], zs_sem.at[k - 1], zr_sem.at[k - 1], z_peers[k - 1])

        def gain_x(e, row):
            return _send(dg_s, dg_x.at[row], xs_sem.at[e - 1], xr_sem.at[e - 1], device((me + e) % groups))

        gain_own = pltpu.make_async_copy(dg_any, dg_z.at[tp], zo_sem)

        def each_near(act):
            for gap in (2, 1):
                for to in (tp + gap, tp - gap):
                    @pl.when((to >= 0) & (to < n_tp))
                    def _():
                        getattr(hid(to), act)()

        @pl.when((j == 0) & (i == 0))
        def _():
            init(0).start()
            gain_own.start()
            _meet(z_peers + [device((me + e) % groups) for e in range(1, groups)])
            for k in range(1, n_tp):
                gain_z(k, tp).start()
            each_near('start')

        @pl.when((j == 1) & (i == 0))
        def _():
            gain_own.wait()
            for k in range(1, n_tp):
                gain_z(k, tp).wait_send()
                gain_z(k, (tp + n_tp - k) % n_tp).wait_recv()
            total = dg_z[0]
            for k in range(1, n_tp):
                total = total + dg_z[k]
            dg_s[...] = total
            dg_x[me] = total

        @pl.when((j == 1) & (i == n_tok - 1))
        def _():
            for e in range(1, groups):
                gain_x(e, me).start()

        @pl.when((j == n_f // 2 + 1) & (i == 0))
        def _():
            @pl.when(tp == 2)
            def _():
                relay(0, 3).wait_recv()
                relay(0, 3).start()

            @pl.when(tp == 1)
            def _():
                relay(3, 0).wait_recv()
                relay(3, 0).start()

        @pl.when(i == 0)
        def _():
            init(j).wait()

        @pl.when(i == n_tok // 2)
        def _():
            @pl.when(j >= 1)
            def _():
                own(j - 1).wait()
                swap(j - 1, core).wait_send()

            @pl.when(j < n_f - 1)
            def _():
                init(j + 1).start()

        first = tp * split.vocab + (core * n_f + j) * COLS
        acc[slot] += _part(x_ref[...], meta_ref, w_ref[...], first)

        @pl.when(i == n_tok - 1)
        def _():
            own(j).start()
            swap(j, core).start()

        @pl.when((j == n_f - 1) & (i == n_tok - 1))
        def _():
            for e in range(1, groups):
                gain_x(e, me).wait_send()
                gain_x(e, (me + groups - e) % groups).wait_recv()
            total = dg_x[0]
            for e in range(1, groups):
                total = total + dg_x[e]
            dg_ref[...] = total
            own(j).wait()
            swap(j, core).wait_send()
            for jj in range(n_f):
                swap(jj, 1 - core).wait_recv()
            each_near('wait_send')

            @pl.when((tp == 1) | (tp == 2))
            def _():
                relay(0, 0).wait_send()

            for row in range(n_tp):
                relayed = ((tp == 2) & (row == 0)) | ((tp == 1) & (row == 3))

                @pl.when((row != tp) & jnp.logical_not(relayed))
                def _():
                    relay(row, tp).wait_recv()

    return pl.pallas_call(
        kernel,
        grid=(n_f, n_tok),
        out_shape=[jax.ShapeDtypeStruct((width, 2 * n_f * COLS), F32), jax.ShapeDtypeStruct((n_tp, sub, width), F32), jax.ShapeDtypeStruct((8, width), F32)],
        in_specs=[
            pl.BlockSpec((TOK, width), lambda j, i: (n_tok + i, 0)),
            pl.BlockSpec((TOK // half, 8, half), lambda j, i: (i, 0, 1)),
            pl.BlockSpec((width, COLS), lambda j, i: (0, lax.axis_index('dp') % 2 * n_f + j)),
            _any(),
            _any(),
            _any(),
        ],
        out_specs=[_any(), _any(), _whole((8, width))],
        scratch_shapes=[pltpu.VMEM((2, width, COLS), F32), pltpu.VMEM((n_tp, 8, width), F32), pltpu.VMEM((8, width), F32), pltpu.VMEM((groups, 8, width), F32)]
        + [pltpu.SemaphoreType.DMA((2,))] * 3 + [pltpu.SemaphoreType.DMA((n_f,)), pltpu.SemaphoreType.DMA((n_tp,)), pltpu.SemaphoreType.DMA((n_tp,)), pltpu.SemaphoreType.DMA]
        + [pltpu.SemaphoreType.DMA((n_tp - 1,))] * 2 + [pltpu.SemaphoreType.DMA] + [pltpu.SemaphoreType.DMA((groups - 1,))] * 2,
        compiler_params=_params(collective_id=4, has_side_effects=True),
        cost_estimate=_cost(4 * rows * width * n_f * COLS, n_f * rows * width * 2),
    )(x, meta, w, part, d_hid, d_gain)


def _head_r(x, meta, w, head_f, head_g, split):
    rows, width = x.shape
    half = meta.shape[2] // 2
    vocab, groups = split.vocab, split.groups
    steps = 2 * groups
    f_wide, r_wide = split.g0 * COLS, 2 * COLS
    strip = width // steps

    def kernel(x_ref, meta_ref, w_ref, f_any, g_any, out_any, acc, f_buf, g_buf, own_sem, in_sem, out_sem):
        i = pl.program_id(0)
        own = pltpu.make_async_copy(acc, out_any.at[:, pl.ds(split.r0 * COLS, r_wide)], own_sem)

        def places(s):
            at = pl.ds(pl.multiple_of(s * strip, 8), strip)
            g_from = pl.ds(pl.multiple_of(s * (width // 2), 8), width // 2)
            g_rows = pl.ds(pl.multiple_of(s % 2 * (width // 2), 8), width // 2)
            g_cols = pl.ds(pl.multiple_of((split.g0 + s // 2) * COLS, COLS), COLS)
            return f_any.at[at], out_any.at[at, pl.ds(0, f_wide)], g_any.at[g_from], out_any.at[g_rows, g_cols]

        def load(s):
            f_src, _, g_src, _ = places(s)
            return (pltpu.make_async_copy(f_src, f_buf.at[s % 2], in_sem.at[0, s % 2]),
                    pltpu.make_async_copy(g_src, g_buf.at[s % 2], in_sem.at[1, s % 2]))

        def store(s):
            _, f_dst, _, g_dst = places(s)
            return (pltpu.make_async_copy(f_buf.at[s % 2], f_dst, out_sem.at[0, s % 2]),
                    pltpu.make_async_copy(g_buf.at[s % 2], g_dst, out_sem.at[1, s % 2]))

        def each(copies, act):
            for c in copies:
                getattr(c, act)()

        @pl.when(i == 0)
        def _():
            each(load(0), 'start')
            acc[...] = jnp.zeros_like(acc)

        @pl.when(i >= 1)
        def _():
            each(load(i - 1), 'wait')
            each(store(i - 1), 'start')

            @pl.when(i >= 2)
            def _():
                each(store(i - 2), 'wait')

            each(load(i), 'start')

        acc[...] += _part(x_ref[...], meta_ref, w_ref[...], lax.axis_index('tp') * vocab + split.r0 * COLS)

        @pl.when(i == steps - 1)
        def _():
            own.start()
            each(load(i), 'wait')
            each(store(i), 'start')
            each(store(i - 1), 'wait')
            each(store(i), 'wait')
            own.wait()

    return pl.pallas_call(
        kernel,
        grid=(steps,),
        out_shape=jax.ShapeDtypeStruct((width, vocab), F32),
        in_specs=[
            pl.BlockSpec((half, width), lambda i: (i, 0)),
            pl.BlockSpec((1, 8, half), lambda i: (i % groups, 0, i // groups)),
            pl.BlockSpec((width, r_wide), lambda i: (0, split.r0 // 2)),
            _any(),
            _any(),
        ],
        out_specs=_any(),
        scratch_shapes=[pltpu.VMEM((width, r_wide), F32), pltpu.VMEM((2, strip, f_wide), F32), pltpu.VMEM((2, width // 2, COLS), F32)]
        + [pltpu.SemaphoreType.DMA] + [pltpu.SemaphoreType.DMA((2, 2))] * 2,
        compiler_params=_params(),
        cost_estimate=_cost(4 * rows * width * r_wide, width * vocab * 8),
    )(x, meta, w, head_f, head_g)


def _finish(hidden, d_x_norm, got, gain, n_tp):
    rows, width = hidden.shape
    sub = rows // n_tp
    step = 64
    n = sub // step

    def kernel(h_ref, own_ref, got_ref, g_ref, dh_ref, dg_ref):
        @pl.when(pl.program_id(0) == 0)
        def _():
            dg_ref[...] = jnp.zeros_like(dg_ref)

        h = h_ref[...].astype(F32)
        inv_rms = lax.rsqrt(jnp.mean(h * h, axis=-1, keepdims=True) + NORM_EPS)
        x = h * inv_rms
        d = own_ref[...]
        tp = lax.axis_index('tp')
        for q in range(n_tp):
            d = d + jnp.where((q != tp) & (q - tp < 3) & (tp - q < 3), got_ref[q], 0.0)
        dg_ref[0:1] += jnp.sum(d * x, axis=0, keepdims=True)
        d_x = d * g_ref[...]
        dh_ref[...] = (inv_rms * (d_x - x * jnp.mean(d_x * x, axis=-1, keepdims=True))).astype(BF16).astype(F32)

    return pl.pallas_call(
        kernel,
        grid=(n,),
        out_shape=[jax.ShapeDtypeStruct((sub, width), F32), jax.ShapeDtypeStruct((8, width), F32)],
        in_specs=[
            pl.BlockSpec((step, width), lambda i: (lax.axis_index('tp') * n + i, 0)),
            pl.BlockSpec((step, width), lambda i: (lax.axis_index('tp') * n + i, 0)),
            pl.BlockSpec((n_tp, step, width), lambda i: (0, i, 0)),
            _whole((1, width)),
        ],
        out_specs=[pl.BlockSpec((step, width), lambda i: (i, 0)), _whole((8, width))],
        compiler_params=_params(),
        cost_estimate=_cost(sub * width * 256, sub * width * 24),
    )(hidden, d_x_norm, got, gain)


def _join(own, got, n_tp):
    sub, width = own.shape

    def kernel(own_ref, got_ref, o_ref):
        o_ref[...] = jnp.where(pl.program_id(0) == lax.axis_index('tp'), own_ref[...], got_ref[0]).astype(BF16)

    return pl.pallas_call(
        kernel,
        grid=(n_tp,),
        out_shape=jax.ShapeDtypeStruct((n_tp * sub, width), BF16),
        in_specs=[_whole((sub, width)), pl.BlockSpec((1, sub, width), lambda q: (q, 0, 0))],
        out_specs=pl.BlockSpec((sub, width), lambda q: (q, 0)),
        compiler_params=_params(),
        cost_estimate=_cost(n_tp * sub * width * 256, n_tp * sub * width * 6),
    )(own, got)


def solution(mesh):
    n_tp, n_cp, n_dp = mesh.shape['tp'], mesh.shape['cp'], mesh.shape['dp']
    groups = n_cp * n_dp

    def part_fn(hidden, tokens, seq_lens, norm_gain, w_head):
        n_seq, local_len, width = hidden.shape
        n_tok = n_seq * local_len
        seg_len = local_len // 2
        split = _Split(w_head.shape[1], groups)
        cp_rank = lax.axis_index('cp')
        gain = norm_gain.reshape(1, width)
        hidden_rows = hidden.reshape(n_tok, width)

        x_norm, send_a, send_b = _norm(hidden_rows, gain)
        x_a = lax.all_gather(send_a, ('cp', 'dp'), axis=0, tiled=True)
        x_b = lax.all_gather(send_b, ('cp', 'dp'), axis=0, tiled=True)

        edge = lax.ppermute(jnp.where(cp_rank == 0, tokens[:, seg_len], tokens[:, 0]), 'cp', [(0, 1), (1, 0)])
        first_end = jnp.where(cp_rank == 0, edge, tokens[:, seg_len])
        second_end = jnp.where(cp_rank == 0, 0, edge)
        labels = jnp.concatenate([tokens[:, 1:seg_len], first_end[:, None], tokens[:, seg_len + 1:], second_end[:, None]], axis=1)
        seg_pos = jnp.arange(seg_len)
        positions = jnp.concatenate([cp_rank * seg_len + seg_pos, (2 * n_cp - 1 - cp_rank) * seg_len + seg_pos])
        valid = (positions[None, :] + 1 < seq_lens[:, None]).astype(F32)
        row = jnp.concatenate([labels.astype(F32).reshape(1, n_tok), valid.reshape(1, n_tok), jnp.zeros((6, n_tok), F32)])
        count = jnp.broadcast_to(jnp.sum(seq_lens - 1).astype(F32), (8, 128))

        logits, meta_row, meta_col = _logits(x_norm, row, count, w_head, n_tp, n_dp)
        d_x_norm, meta = _d_norm(logits, meta_col, meta_row, w_head, n_cp, n_dp)
        tok_loss = meta_row[3].reshape(n_seq, local_len)
        loss_mean = jnp.sum(meta[:, 3]) / meta[0, 4, 0]
        meta, tok_loss, loss_mean = lax.optimization_barrier((meta, tok_loss, loss_mean))
        part, x_all, got = _head_a(x_a, meta, w_head, d_x_norm, split, n_tp, n_dp)
        d_hid, d_gain = _finish(hidden_rows, d_x_norm, got, gain, n_tp)
        d_head_g, x_all = _head_g(x_b, meta, w_head, part, x_all, split, n_dp)
        d_head_g = lax.all_gather(d_head_g, ('cp', 'dp'), axis=0, tiled=True)
        d_head_f, d_hid_all, d_gain = _head_f(x_all, meta, w_head, part, d_hid, d_gain, split, n_tp, n_cp, n_dp)
        d_hidden = _join(d_hid, d_hid_all, n_tp)
        d_head = _head_r(x_all, meta, w_head, d_head_f, d_head_g, split)
        return tok_loss, loss_mean, d_hidden.reshape(hidden.shape), d_gain[0], d_head

    return jax.shard_map(part_fn, mesh=mesh, in_specs=(P('dp', 'cp', None), P('dp', 'cp'), P('dp'), P(None), P(None, 'tp')), out_specs=(P('dp', 'cp'), P(), P('dp', 'cp', None), P(None), P(None, 'tp')), check_vma=False)
```

```python
import jax
import jax.numpy as jnp
from jax import lax
from jax.sharding import PartitionSpec as P
from jax.experimental import pallas as pl
from jax.experimental.pallas import tpu as pltpu

NORM_EPS = 1e-5
F32, BF16 = jnp.float32, jnp.bfloat16
COLS = 512
TOK = 1024
VMEM = 63_000_000
MESH = pl.DeviceIdType.MESH


def _params(**kw):
    return pltpu.CompilerParams(vmem_limit_bytes=VMEM, **kw)


def _cost(flops, bytes_accessed):
    return pl.CostEstimate(flops=int(flops), bytes_accessed=int(bytes_accessed), transcendentals=0)


def _any():
    return pl.BlockSpec(memory_space=pl.ANY)


def _whole(shape):
    return pl.BlockSpec(shape, lambda *ids: (0,) * len(shape))


def _meet(peers):
    barrier = pltpu.get_barrier_semaphore()
    for peer in peers:
        pl.semaphore_signal(barrier, inc=1, device_id=peer, device_id_type=MESH)
    pl.semaphore_wait(barrier, len(peers))


def _send(src, dst, send_sem, recv_sem, peer):
    return pltpu.make_async_remote_copy(src, dst, send_sem, recv_sem, device_id=peer, device_id_type=MESH)


def _plane(n_dp):
    me = lax.axis_index('cp') * n_dp + lax.axis_index('dp')
    return me, lambda p: {'cp': p // n_dp, 'dp': p % n_dp}


def _columns(rows):
    return jnp.concatenate([rows, jnp.zeros((120, rows.shape[1]), F32)], axis=0).T


def _norm(hidden, gain, half, x_norm=None):
    rows, width = hidden.shape
    step = 128
    n = rows // 2 // step

    def kernel(h_ref, g_ref, *refs):
        x_ref, xs_ref = refs[-2:]
        h = h_ref[...].astype(F32)
        inv_rms = lax.rsqrt(jnp.mean(h * h, axis=-1, keepdims=True) + NORM_EPS)
        x = (h * inv_rms * g_ref[...]).astype(BF16)
        x_ref[...] = x
        xs_ref[...] = x.astype(F32)

    at = pl.BlockSpec((step, width), lambda i: (half * n + i, 0))
    return pl.pallas_call(
        kernel,
        grid=(n,),
        out_shape=[jax.ShapeDtypeStruct((rows, width), BF16), jax.ShapeDtypeStruct((rows // 2, width), F32)],
        in_specs=[at, _whole((1, width))] + [_any()] * (x_norm is not None),
        out_specs=[at, pl.BlockSpec((step, width), lambda i: (i, 0))],
        input_output_aliases={2: 0} if x_norm is not None else {},
        compiler_params=_params(),
        cost_estimate=_cost(rows * width * 128, rows * width * 4),
    )(*((hidden, gain) if x_norm is None else (hidden, gain, x_norm)))


def _logits(x, row, count, w, n_tp, n_dp):
    rows, width = x.shape
    vocab = w.shape[1]
    cols = 1024
    steps = vocab // cols

    def kernel(x_ref, row_ref, cnt_ref, cnt_any, w_ref, z_ref, mrow_ref, mcol_ref, m_ref, s_ref, t_ref, lab_ref, st_buf, cnt_buf, cs_sem, cr_sem, ss_sem, sr_sem):
        i = pl.program_id(0)
        tp, dp = lax.axis_index('tp'), lax.axis_index('dp')

        def tell(k):
            return _send(cnt_any, cnt_buf.at[k - 1], cs_sem.at[k - 1], cr_sem.at[k - 1], {'dp': (dp + k) % n_dp})

        def give(k, slot):
            return _send(st_buf.at[slot], st_buf.at[slot], ss_sem.at[k - 1], sr_sem.at[k - 1], {'tp': (tp + k) % n_tp})

        @pl.when(i == 0)
        def _():
            _meet([{'tp': (tp + k) % n_tp} for k in range(1, n_tp)] + [{'dp': (dp + k) % n_dp} for k in range(1, n_dp)])
            for k in range(1, n_dp):
                tell(k).start()
            m_ref[...] = jnp.full_like(m_ref, -jnp.inf)
            s_ref[...] = jnp.zeros_like(s_ref)
            t_ref[...] = jnp.zeros_like(t_ref)
            lab_ref[...] = _columns(row_ref[...])

        z = jnp.dot(x_ref[...], w_ref[...], preferred_element_type=F32)
        z_ref[...] = z
        rel = lab_ref[:, 0:1].astype(jnp.int32) - (tp * vocab + cols * i)
        lane = lax.broadcasted_iota(jnp.int32, (rows, 128), 1)
        old = m_ref[...]
        top = old
        for g in range(cols // 128):
            top = jnp.maximum(top, z[:, g * 128:(g + 1) * 128])
        total = s_ref[...] * jnp.exp(old - top)
        target = t_ref[...]
        for g in range(cols // 128):
            z_g = z[:, g * 128:(g + 1) * 128]
            total = total + jnp.exp(z_g - top)
            target = target + jnp.where(lane == rel - g * 128, z_g, 0.0)
        m_ref[...] = top
        s_ref[...] = total
        t_ref[...] = target

        @pl.when(i == steps - 1)
        def _():
            top, total = m_ref[...], s_ref[...]
            row_max = jnp.max(top, axis=1, keepdims=True)
            row_sum = jnp.sum(total * jnp.exp(top - row_max), axis=1, keepdims=True)
            row_target = jnp.sum(t_ref[...], axis=1, keepdims=True)
            st_buf[tp] = jnp.where(lane == 0, row_max, jnp.where(lane == 1, row_sum, row_target)).T[0:8]
            for k in range(1, n_dp):
                tell(k).wait()
            for k in range(1, n_tp):
                give(k, tp).start()
            n_valid = cnt_ref[0:1, 0:1]
            for k in range(1, n_dp):
                n_valid = n_valid + cnt_buf[k - 1, 0:1, 0:1]
            for k in range(1, n_tp):
                give(k, tp).wait_send()
                give(k, (tp + n_tp - k) % n_tp).wait_recv()
            top = st_buf[0, 0:1]
            for k in range(1, n_tp):
                top = jnp.maximum(top, st_buf[k, 0:1])
            total = st_buf[0, 1:2] * jnp.exp(st_buf[0, 0:1] - top)
            target = st_buf[0, 2:3]
            for k in range(1, n_tp):
                total = total + st_buf[k, 1:2] * jnp.exp(st_buf[k, 0:1] - top)
                target = target + st_buf[k, 2:3]
            lse = top + jnp.log(total)
            valid = row_ref[1:2]
            sub = lax.broadcasted_iota(jnp.int32, (8, rows), 0)
            meta = jnp.where(sub == 0, lse, jnp.where(sub == 1, row_ref[0:1], jnp.where(sub == 2, valid / n_valid, jnp.where(sub == 3, (lse - target) * valid, n_valid))))
            mrow_ref[...] = meta
            mcol_ref[...] = _columns(meta)

    return pl.pallas_call(
        kernel,
        grid=(steps,),
        out_shape=[jax.ShapeDtypeStruct((rows, vocab), F32), jax.ShapeDtypeStruct((8, rows), F32), jax.ShapeDtypeStruct((rows, 128), F32)],
        in_specs=[_whole((rows, width)), _whole((8, rows)), _whole((8, 128)), _any(), pl.BlockSpec((width, cols), lambda i: (0, i))],
        out_specs=[pl.BlockSpec((rows, cols), lambda i: (0, i)), _whole((8, rows)), _whole((rows, 128))],
        scratch_shapes=[pltpu.VMEM((rows, 128), F32)] * 4
        + [pltpu.VMEM((n_tp, 8, rows), F32), pltpu.VMEM((n_dp - 1, 8, 128), F32)]
        + [pltpu.SemaphoreType.DMA((n_dp - 1,))] * 2 + [pltpu.SemaphoreType.DMA((n_tp - 1,))] * 2,
        compiler_params=_params(collective_id=1, has_side_effects=True),
        cost_estimate=_cost(2 * rows * width * vocab, vocab * (2 * width + 4 * rows)),
    )(x, row, count, count, w)


def _d_logits(z, meta, first):
    rel = meta[:, 1:2].astype(jnp.int32) - first
    hit = lax.broadcasted_iota(jnp.int32, z.shape, 1) == rel
    return ((jnp.exp(z - meta[:, 0:1]) - jnp.where(hit, 1.0, 0.0)) * meta[:, 2:3]).astype(BF16)


def _d_norm(z, mcol, mrow, w, n_cp, n_dp):
    rows, vocab = z.shape
    width = w.shape[0]
    cols = 1024
    steps = vocab // cols
    groups = n_cp * n_dp

    def kernel(z_ref, mcol_ref, mrow_any, w_ref, acc_ref, all_ref, buf, own_sem, send_sem, recv_sem):
        i = pl.program_id(0)
        me, device = _plane(n_dp)
        own = pltpu.make_async_copy(mrow_any, buf.at[me], own_sem)

        def give(e, slot):
            return _send(mrow_any, buf.at[slot], send_sem.at[e - 1], recv_sem.at[e - 1], device((me + e) % groups))

        @pl.when(i == 0)
        def _():
            own.start()
            _meet([device((me + e) % groups) for e in range(1, groups)])
            for e in range(1, groups):
                give(e, me).start()
            acc_ref[...] = jnp.zeros_like(acc_ref)

        d = _d_logits(z_ref[...], mcol_ref[...], lax.axis_index('tp') * vocab + i * cols)
        acc_ref[...] += lax.dot_general(d, w_ref[...], (((1,), (1,)), ((), ())), preferred_element_type=F32)

        @pl.when(i == steps - 1)
        def _():
            own.wait()
            for e in range(1, groups):
                give(e, me).wait_send()
                give(e, (me + groups - e) % groups).wait_recv()
            all_ref[...] = buf[...]

    return pl.pallas_call(
        kernel,
        grid=(steps,),
        out_shape=[jax.ShapeDtypeStruct((rows, width), F32), jax.ShapeDtypeStruct((groups, 8, rows), F32)],
        in_specs=[pl.BlockSpec((rows, cols), lambda i: (0, i)), _whole((rows, 128)), _any(), pl.BlockSpec((width, cols), lambda i: (0, i))],
        out_specs=[_whole((rows, width)), _whole((groups, 8, rows))],
        scratch_shapes=[pltpu.VMEM((groups, 8, rows), F32), pltpu.SemaphoreType.DMA] + [pltpu.SemaphoreType.DMA((groups - 1,))] * 2,
        compiler_params=_params(collective_id=2, has_side_effects=True),
        cost_estimate=_cost(2 * rows * width * vocab, vocab * (2 * width + 4 * rows)),
    )(z, mcol, mrow, w)


class _Split:
    def __init__(self, vocab, groups):
        self.vocab, self.groups = vocab, groups
        self.blocks = vocab // COLS
        self.n_f = (self.blocks - groups - 2) // 2
        self.g0 = 2 * self.n_f
        self.r0 = self.g0 + groups
        self.n = 1 + self.n_f

    def block(self, b, me, core):
        return jnp.where(b == 0, self.g0 + me, core * self.n_f + b - 1)


def _part(x_b, meta, w, first):
    rows = jnp.concatenate([meta[k] for k in range(meta.shape[0])], axis=1) if meta.shape[0] > 1 else meta[0]
    d = _d_logits(jnp.dot(x_b, w, preferred_element_type=F32), _columns(rows), first)
    return lax.dot_general(x_b, d, (((0,), (0,)), ((), ())), preferred_element_type=F32)


def _head_a(x, meta, w, d_x_norm, split, n_tp, n_dp):
    rows, width = x.shape
    half = meta.shape[2] // 2
    n_tok = rows // TOK
    sub = d_x_norm.shape[0] // n_tp

    def kernel(x_ref, meta_ref, w_ref, dx_any, acc_ref, xb_ref, got_any, leg, mid, send_sem, recv_sem, leg_sem, mid_sem):
        b, i = pl.program_id(0), pl.program_id(1)
        step = b * n_tok + i
        stage = [split.n * n_tok * part // 32 for part in (10, 12)]
        tp = lax.axis_index('tp')
        me, _ = _plane(n_dp)
        inner = (tp == 1) | (tp == 2)
        far = jnp.where(tp < 2, 3, 0)

        def quarter(q):
            return dx_any.at[pl.ds(pl.multiple_of(q * sub, 8), sub)]

        def give(to, src):
            return _send(src, got_any.at[tp], send_sem.at[to], recv_sem.at[tp], {'tp': to})

        def arrive(frm):
            return _send(mid, got_any.at[frm], send_sem.at[frm], recv_sem.at[frm], {'tp': frm})

        first_leg = _send(quarter(far), leg, leg_sem.at[0], leg_sem.at[1], {'tp': jnp.where(tp == 0, 1, 2)})
        load_mid = pltpu.make_async_copy(quarter(far), mid, mid_sem)

        @pl.when((b == 0) & (i == 0))
        def _():
            _meet([{'tp': (tp + k) % n_tp} for k in range(1, n_tp)])

            @pl.when(inner)
            def _():
                load_mid.start()
                give(3 - tp, quarter(3 - tp)).start()
                give(3 - far, quarter(3 - far)).start()

            @pl.when(jnp.logical_not(inner))
            def _():
                first_leg.start()

        @pl.when((step == stage[0]) & jnp.logical_not(inner))
        def _():
            for gap in (1, 2):
                to = jnp.where(tp == 0, gap, 3 - gap)
                give(to, quarter(to)).start()

        @pl.when((step == stage[1]) & inner)
        def _():
            load_mid.wait()
            first_leg.wait_recv()
            mid[...] += leg[...]

        @pl.when((step == stage[1] + 1) & inner)
        def _():
            give(far, mid).start()

        @pl.when(i == 0)
        def _():
            acc_ref[...] = jnp.zeros_like(acc_ref)

        x_b = x_ref[...].astype(BF16)

        @pl.when(b == 0)
        def _():
            xb_ref[...] = x_b

        first = tp * split.vocab + split.block(b, me, lax.axis_index('dp') % 2) * COLS
        acc_ref[...] += _part(x_b, meta_ref, w_ref[...], first)

        @pl.when((b == split.n - 1) & (i == n_tok - 1))
        def _():
            @pl.when(inner)
            def _():
                for q in range(n_tp):
                    @pl.when(tp != q)
                    def _():
                        give(q, mid).wait_send()
                        arrive(q).wait_recv()

            @pl.when(jnp.logical_not(inner))
            def _():
                first_leg.wait_send()
                for q in (1, 2):
                    give(q, mid).wait_send()
                    arrive(q).wait_recv()

    return pl.pallas_call(
        kernel,
        grid=(split.n, n_tok),
        out_shape=[jax.ShapeDtypeStruct((width, split.n * COLS), F32), jax.ShapeDtypeStruct((2 * rows, width), BF16), jax.ShapeDtypeStruct((n_tp, sub, width), F32)],
        in_specs=[
            pl.BlockSpec((TOK, width), lambda b, i: (i, 0)),
            pl.BlockSpec((TOK // half, 8, half), lambda b, i: (i, 0, 0)),
            pl.BlockSpec((width, COLS), lambda b, i: (0, split.block(b, _plane(n_dp)[0], lax.axis_index('dp') % 2))),
            _any(),
        ],
        out_specs=[pl.BlockSpec((width, COLS), lambda b, i: (0, b)), pl.BlockSpec((TOK, width), lambda b, i: (jnp.where(b == 0, i, n_tok - 1), 0)), _any()],
        scratch_shapes=[pltpu.VMEM((sub, width), F32)] * 2 + [pltpu.SemaphoreType.DMA((n_tp,))] * 2 + [pltpu.SemaphoreType.DMA((2,)), pltpu.SemaphoreType.DMA],
        compiler_params=_params(collective_id=3, has_side_effects=True),
        cost_estimate=_cost(4 * rows * width * split.n * COLS, split.n * rows * width * 4),
    )(x, meta, w, d_x_norm)


def _head_g(x, meta, w, part, x_all, split, n_dp):
    rows, width = x.shape
    half = meta.shape[2] // 2
    n_tok = rows // half

    def kernel(x_ref, meta_ref, w_ref, init_ref, _, acc_ref, xb_ref):
        @pl.when(pl.program_id(0) == 0)
        def _():
            acc_ref[...] = init_ref[...]

        x_b = x_ref[...].astype(BF16)
        xb_ref[...] = x_b
        first = lax.axis_index('tp') * split.vocab + (split.g0 + _plane(n_dp)[0]) * COLS
        acc_ref[...] += _part(x_b, meta_ref, w_ref[...], first)

    return pl.pallas_call(
        kernel,
        grid=(n_tok,),
        out_shape=[jax.ShapeDtypeStruct((width, COLS), F32), jax.ShapeDtypeStruct((2 * rows, width), BF16)],
        in_specs=[
            pl.BlockSpec((half, width), lambda i: (i, 0)),
            pl.BlockSpec((1, 8, half), lambda i: (i, 0, 1)),
            pl.BlockSpec((width, COLS), lambda i: (0, split.g0 + _plane(n_dp)[0])),
            _whole((width, COLS)),
            _any(),
        ],
        out_specs=[_whole((width, COLS)), pl.BlockSpec((half, width), lambda i: (n_tok + i, 0))],
        input_output_aliases={4: 1},
        compiler_params=_params(),
        cost_estimate=_cost(4 * rows * width * COLS, rows * width * 6),
    )(x, meta, w, part, x_all)


def _head_f(x, meta, w, part, d_hid, d_gain, split, n_tp, n_cp, n_dp):
    width = x.shape[1]
    rows = x.shape[0] // 2
    half = meta.shape[2] // 2
    n_f, groups = split.n_f, n_cp * n_dp
    n_tok = rows // TOK
    sub = d_hid.shape[0]

    def kernel(x_ref, meta_ref, w_ref, init_any, dh_any, dg_any, out_any, dhall_any, dg_ref, acc, dg_z, dg_s, dg_x, init_sem, own_sem, send_sem, recv_sem, hs_sem, hr_sem, fs_sem, zs_sem, zr_sem, zo_sem, xs_sem, xr_sem):
        j, i = pl.program_id(0), pl.program_id(1)
        step = j * n_tok + i
        stage = [n_f * n_tok * part // 28 for part in (9, 12, 18, 21)]
        tp, dp = lax.axis_index('tp'), lax.axis_index('dp')
        inner = (tp == 1) | (tp == 2)
        me, device = _plane(n_dp)
        core = dp % 2
        slot = j % 2
        z_peers = [{'tp': (tp + k) % n_tp} for k in range(1, n_tp)]

        def at(owner, jj):
            return out_any.at[:, pl.ds(pl.multiple_of((owner * n_f + jj) * COLS, COLS), COLS)]

        def init(jj):
            return pltpu.make_async_copy(init_any.at[:, pl.ds(pl.multiple_of((jj + 1) * COLS, COLS), COLS)], acc.at[jj % 2], init_sem.at[jj % 2])

        def own(jj):
            return pltpu.make_async_copy(acc.at[jj % 2], at(core, jj), own_sem.at[jj % 2])

        def swap(jj, owner):
            return _send(acc.at[jj % 2], at(owner, jj), send_sem.at[jj % 2], recv_sem.at[jj], {'dp': dp + 1 - 2 * core})

        def hid(to, h):
            rows_h = pl.ds(h * (sub // 2), sub // 2)
            return _send(dh_any.at[rows_h], dhall_any.at[tp, rows_h], hs_sem.at[to, h], hr_sem.at[tp, h], {'tp': to})

        def relay(row, to, h):
            at_h = dhall_any.at[row, pl.ds(h * (sub // 2), sub // 2)]
            return _send(at_h, at_h, fs_sem.at[h], hr_sem.at[row, h], {'tp': to})

        def gain_z(k, row):
            return _send(dg_any, dg_z.at[row], zs_sem.at[k - 1], zr_sem.at[k - 1], z_peers[k - 1])

        def gain_x(e, row):
            return _send(dg_s, dg_x.at[row], xs_sem.at[e - 1], xr_sem.at[e - 1], device((me + e) % groups))

        gain_own = pltpu.make_async_copy(dg_any, dg_z.at[tp], zo_sem)

        def across(h, act):
            getattr(hid(jnp.where(tp < 2, tp + 2, tp - 2), h), act)()

        def beside(inward, act):
            for h in range(2):
                getattr(hid(jnp.where((tp < 2) == inward, tp + 1, tp - 1), h), act)()

        def pass_on(h):
            relay(3 * (2 - tp), 3 * (tp - 1), h).wait_recv()
            relay(3 * (2 - tp), 3 * (tp - 1), h).start()

        @pl.when((j == 0) & (i == 0))
        def _():
            init(0).start()
            gain_own.start()
            _meet(z_peers + [device((me + e) % groups) for e in range(1, groups)])
            for k in range(1, n_tp):
                gain_z(k, tp).start()
            across(0, 'start')

            @pl.when(inner)
            def _():
                beside(False, 'start')

        @pl.when(step == stage[0])
        def _():
            across(1, 'start')

        @pl.when((step == stage[1]) & inner)
        def _():
            pass_on(0)

        @pl.when(step == stage[2])
        def _():
            beside(True, 'start')

        @pl.when((step == stage[3]) & inner)
        def _():
            pass_on(1)

        @pl.when((j == 1) & (i == 0))
        def _():
            gain_own.wait()
            for k in range(1, n_tp):
                gain_z(k, tp).wait_send()
                gain_z(k, (tp + n_tp - k) % n_tp).wait_recv()
            total = dg_z[0]
            for k in range(1, n_tp):
                total = total + dg_z[k]
            dg_s[...] = total
            dg_x[me] = total

        @pl.when((j == 1) & (i == n_tok - 1))
        def _():
            for e in range(1, groups):
                gain_x(e, me).start()

        @pl.when(i == 0)
        def _():
            init(j).wait()

        @pl.when(i == n_tok // 2)
        def _():
            @pl.when(j >= 1)
            def _():
                own(j - 1).wait()
                swap(j - 1, core).wait_send()

            @pl.when(j < n_f - 1)
            def _():
                init(j + 1).start()

        first = tp * split.vocab + (core * n_f + j) * COLS
        acc[slot] += _part(x_ref[...], meta_ref, w_ref[...], first)

        @pl.when(i == n_tok - 1)
        def _():
            own(j).start()
            swap(j, core).start()

        @pl.when((j == n_f - 1) & (i == n_tok - 1))
        def _():
            for e in range(1, groups):
                gain_x(e, me).wait_send()
                gain_x(e, (me + groups - e) % groups).wait_recv()
            total = dg_x[0]
            for e in range(1, groups):
                total = total + dg_x[e]
            dg_ref[...] = total
            own(j).wait()
            swap(j, core).wait_send()
            for jj in range(n_f):
                swap(jj, 1 - core).wait_recv()
            for h in range(2):
                across(h, 'wait_send')
            beside(True, 'wait_send')

            @pl.when(inner)
            def _():
                beside(False, 'wait_send')
                for h in range(2):
                    relay(0, 0, h).wait_send()

            for row in range(n_tp):
                relayed = ((tp == 2) & (row == 0)) | ((tp == 1) & (row == 3))

                @pl.when((row != tp) & jnp.logical_not(relayed))
                def _():
                    for h in range(2):
                        relay(row, tp, h).wait_recv()

    return pl.pallas_call(
        kernel,
        grid=(n_f, n_tok),
        out_shape=[jax.ShapeDtypeStruct((width, 2 * n_f * COLS), F32), jax.ShapeDtypeStruct((n_tp, sub, width), F32), jax.ShapeDtypeStruct((8, width), F32)],
        in_specs=[
            pl.BlockSpec((TOK, width), lambda j, i: (n_tok + i, 0)),
            pl.BlockSpec((TOK // half, 8, half), lambda j, i: (i, 0, 1)),
            pl.BlockSpec((width, COLS), lambda j, i: (0, lax.axis_index('dp') % 2 * n_f + j)),
            _any(),
            _any(),
            _any(),
        ],
        out_specs=[_any(), _any(), _whole((8, width))],
        scratch_shapes=[pltpu.VMEM((2, width, COLS), F32), pltpu.VMEM((n_tp, 8, width), F32), pltpu.VMEM((8, width), F32), pltpu.VMEM((groups, 8, width), F32)]
        + [pltpu.SemaphoreType.DMA((2,))] * 3 + [pltpu.SemaphoreType.DMA((n_f,)), pltpu.SemaphoreType.DMA((n_tp, 2)), pltpu.SemaphoreType.DMA((n_tp, 2)), pltpu.SemaphoreType.DMA((2,))]
        + [pltpu.SemaphoreType.DMA((n_tp - 1,))] * 2 + [pltpu.SemaphoreType.DMA] + [pltpu.SemaphoreType.DMA((groups - 1,))] * 2,
        compiler_params=_params(collective_id=4, has_side_effects=True),
        cost_estimate=_cost(4 * rows * width * n_f * COLS, n_f * rows * width * 2),
    )(x, meta, w, part, d_hid, d_gain)


def _head_r(x, meta, w, head_f, head_g, d_hid, d_hid_all, split, n_tp):
    rows, width = x.shape
    half = meta.shape[2] // 2
    vocab, groups = split.vocab, split.groups
    steps = 2 * groups
    f_wide, r_wide = split.g0 * COLS, 2 * COLS
    strip = width // steps
    per_q = steps // n_tp
    sub = d_hid.shape[0]
    piece = sub // per_q

    def kernel(x_ref, meta_ref, w_ref, f_any, g_any, dh_ref, dhall_ref, out_any, hid_ref, acc, f_buf, g_buf, own_sem, in_sem, out_sem):
        i = pl.program_id(0)
        own = pltpu.make_async_copy(acc, out_any.at[:, pl.ds(split.r0 * COLS, r_wide)], own_sem)

        def places(s):
            at = pl.ds(pl.multiple_of(s * strip, 8), strip)
            g_from = pl.ds(pl.multiple_of(s * (width // 2), 8), width // 2)
            g_rows = pl.ds(pl.multiple_of(s % 2 * (width // 2), 8), width // 2)
            g_cols = pl.ds(pl.multiple_of((split.g0 + s // 2) * COLS, COLS), COLS)
            return f_any.at[at], out_any.at[at, pl.ds(0, f_wide)], g_any.at[g_from], out_any.at[g_rows, g_cols]

        def load(s):
            f_src, _, g_src, _ = places(s)
            return (pltpu.make_async_copy(f_src, f_buf.at[s % 2], in_sem.at[0, s % 2]),
                    pltpu.make_async_copy(g_src, g_buf.at[s % 2], in_sem.at[1, s % 2]))

        def store(s):
            _, f_dst, _, g_dst = places(s)
            return (pltpu.make_async_copy(f_buf.at[s % 2], f_dst, out_sem.at[0, s % 2]),
                    pltpu.make_async_copy(g_buf.at[s % 2], g_dst, out_sem.at[1, s % 2]))

        def each(copies, act):
            for c in copies:
                getattr(c, act)()

        @pl.when(i == 0)
        def _():
            each(load(0), 'start')
            acc[...] = jnp.zeros_like(acc)

        @pl.when(i >= 1)
        def _():
            each(load(i - 1), 'wait')
            each(store(i - 1), 'start')

            @pl.when(i >= 2)
            def _():
                each(store(i - 2), 'wait')

            each(load(i), 'start')

        hid_ref[...] = jnp.where(i // per_q == lax.axis_index('tp'), dh_ref[...], dhall_ref[0]).astype(BF16)
        acc[...] += _part(x_ref[...], meta_ref, w_ref[...], lax.axis_index('tp') * vocab + split.r0 * COLS)

        @pl.when(i == steps - 1)
        def _():
            own.start()
            each(load(i), 'wait')
            each(store(i), 'start')
            each(store(i - 1), 'wait')
            each(store(i), 'wait')
            own.wait()

    return pl.pallas_call(
        kernel,
        grid=(steps,),
        out_shape=[jax.ShapeDtypeStruct((width, vocab), F32), jax.ShapeDtypeStruct((n_tp * sub, width), BF16)],
        in_specs=[
            pl.BlockSpec((half, width), lambda i: (i, 0)),
            pl.BlockSpec((1, 8, half), lambda i: (i % groups, 0, i // groups)),
            pl.BlockSpec((width, r_wide), lambda i: (0, split.r0 // 2)),
            _any(),
            _any(),
            pl.BlockSpec((piece, width), lambda i: (i % per_q, 0)),
            pl.BlockSpec((1, piece, width), lambda i: (i // per_q, i % per_q, 0)),
        ],
        out_specs=[_any(), pl.BlockSpec((piece, width), lambda i: (i, 0))],
        scratch_shapes=[pltpu.VMEM((width, r_wide), F32), pltpu.VMEM((2, strip, f_wide), F32), pltpu.VMEM((2, width // 2, COLS), F32)]
        + [pltpu.SemaphoreType.DMA] + [pltpu.SemaphoreType.DMA((2, 2))] * 2,
        compiler_params=_params(),
        cost_estimate=_cost(4 * rows * width * r_wide, width * vocab * 8),
    )(x, meta, w, head_f, head_g, d_hid, d_hid_all)


def _finish(hidden, d_x_norm, got, gain, n_tp):
    rows, width = hidden.shape
    sub = rows // n_tp
    step = 64
    n = sub // step

    def kernel(h_ref, own_ref, got_ref, g_ref, dh_ref, dg_ref):
        @pl.when(pl.program_id(0) == 0)
        def _():
            dg_ref[...] = jnp.zeros_like(dg_ref)

        h = h_ref[...].astype(F32)
        inv_rms = lax.rsqrt(jnp.mean(h * h, axis=-1, keepdims=True) + NORM_EPS)
        x = h * inv_rms
        d = own_ref[...]
        tp = lax.axis_index('tp')
        for q in range(n_tp):
            d = d + jnp.where((q != tp) & (q - tp < 3) & (tp - q < 3), got_ref[q], 0.0)
        dg_ref[0:1] += jnp.sum(d * x, axis=0, keepdims=True)
        d_x = d * g_ref[...]
        dh_ref[...] = (inv_rms * (d_x - x * jnp.mean(d_x * x, axis=-1, keepdims=True))).astype(BF16).astype(F32)

    return pl.pallas_call(
        kernel,
        grid=(n,),
        out_shape=[jax.ShapeDtypeStruct((sub, width), F32), jax.ShapeDtypeStruct((8, width), F32)],
        in_specs=[
            pl.BlockSpec((step, width), lambda i: (lax.axis_index('tp') * n + i, 0)),
            pl.BlockSpec((step, width), lambda i: (lax.axis_index('tp') * n + i, 0)),
            pl.BlockSpec((n_tp, step, width), lambda i: (0, i, 0)),
            _whole((1, width)),
        ],
        out_specs=[pl.BlockSpec((step, width), lambda i: (i, 0)), _whole((8, width))],
        compiler_params=_params(),
        cost_estimate=_cost(sub * width * 256, sub * width * 24),
    )(hidden, d_x_norm, got, gain)


def solution(mesh):
    n_tp, n_cp, n_dp = mesh.shape['tp'], mesh.shape['cp'], mesh.shape['dp']
    groups = n_cp * n_dp

    def part_fn(hidden, tokens, seq_lens, norm_gain, w_head):
        n_seq, local_len, width = hidden.shape
        n_tok = n_seq * local_len
        seg_len = local_len // 2
        split = _Split(w_head.shape[1], groups)
        cp_rank = lax.axis_index('cp')
        gain = norm_gain.reshape(1, width)
        hidden_rows = hidden.reshape(n_tok, width)

        x_norm, send_a = _norm(hidden_rows, gain, 0)
        x_a = lax.all_gather(send_a, ('cp', 'dp'), axis=0, tiled=True)
        x_norm, send_b = _norm(hidden_rows, gain, 1, x_norm)
        x_b = lax.all_gather(send_b, ('cp', 'dp'), axis=0, tiled=True)

        edge = lax.ppermute(jnp.where(cp_rank == 0, tokens[:, seg_len], tokens[:, 0]), 'cp', [(0, 1), (1, 0)])
        first_end = jnp.where(cp_rank == 0, edge, tokens[:, seg_len])
        second_end = jnp.where(cp_rank == 0, 0, edge)
        labels = jnp.concatenate([tokens[:, 1:seg_len], first_end[:, None], tokens[:, seg_len + 1:], second_end[:, None]], axis=1)
        seg_pos = jnp.arange(seg_len)
        positions = jnp.concatenate([cp_rank * seg_len + seg_pos, (2 * n_cp - 1 - cp_rank) * seg_len + seg_pos])
        valid = (positions[None, :] + 1 < seq_lens[:, None]).astype(F32)
        row = jnp.concatenate([labels.astype(F32).reshape(1, n_tok), valid.reshape(1, n_tok), jnp.zeros((6, n_tok), F32)])
        count = jnp.broadcast_to(jnp.sum(seq_lens - 1).astype(F32), (8, 128))

        logits, meta_row, meta_col = _logits(x_norm, row, count, w_head, n_tp, n_dp)
        d_x_norm, meta = _d_norm(logits, meta_col, meta_row, w_head, n_cp, n_dp)
        tok_loss = meta_row[3].reshape(n_seq, local_len)
        loss_mean = jnp.sum(meta[:, 3]) / meta[0, 4, 0]
        meta, tok_loss, loss_mean = lax.optimization_barrier((meta, tok_loss, loss_mean))
        part, x_all, got = _head_a(x_a, meta, w_head, d_x_norm, split, n_tp, n_dp)
        d_head_g, x_all = _head_g(x_b, meta, w_head, part, x_all, split, n_dp)
        got, d_head_g = lax.optimization_barrier((got, d_head_g))
        d_head_g = lax.all_gather(d_head_g, ('cp', 'dp'), axis=0, tiled=True)
        d_hid, d_gain = _finish(hidden_rows, d_x_norm, got, gain, n_tp)
        d_head_f, d_hid_all, d_gain = _head_f(x_all, meta, w_head, part, d_hid, d_gain, split, n_tp, n_cp, n_dp)
        d_head, d_hidden = _head_r(x_all, meta, w_head, d_head_f, d_head_g, d_hid, d_hid_all, split, n_tp)

        return tok_loss, loss_mean, d_hidden.reshape(hidden.shape), d_gain[0], d_head

    return jax.shard_map(part_fn, mesh=mesh, in_specs=(P('dp', 'cp', None), P('dp', 'cp'), P('dp'), P(None), P(None, 'tp')), out_specs=(P('dp', 'cp'), P(), P('dp', 'cp', None), P(None), P(None, 'tp')), check_vma=False)
```

```python
import jax
import jax.numpy as jnp
from jax import lax
from jax.sharding import PartitionSpec as P
from jax.experimental import pallas as pl
from jax.experimental.pallas import tpu as pltpu

NORM_EPS = 1e-5
F32, BF16 = jnp.float32, jnp.bfloat16
COLS = 512
TOK = 1024
VMEM = 63_000_000
MESH = pl.DeviceIdType.MESH


def _params(**kw):
    return pltpu.CompilerParams(vmem_limit_bytes=VMEM, **kw)


def _cost(flops, bytes_accessed):
    return pl.CostEstimate(flops=int(flops), bytes_accessed=int(bytes_accessed), transcendentals=0)


def _any():
    return pl.BlockSpec(memory_space=pl.ANY)


def _whole(shape):
    return pl.BlockSpec(shape, lambda *ids: (0,) * len(shape))


def _meet(peers):
    barrier = pltpu.get_barrier_semaphore()
    for peer in peers:
        pl.semaphore_signal(barrier, inc=1, device_id=peer, device_id_type=MESH)
    pl.semaphore_wait(barrier, len(peers))


def _send(src, dst, send_sem, recv_sem, peer):
    return pltpu.make_async_remote_copy(src, dst, send_sem, recv_sem, device_id=peer, device_id_type=MESH)


def _plane(n_dp):
    me = lax.axis_index('cp') * n_dp + lax.axis_index('dp')
    return me, lambda p: {'cp': p // n_dp, 'dp': p % n_dp}


def _columns(rows):
    return jnp.concatenate([rows, jnp.zeros((120, rows.shape[1]), F32)], axis=0).T


def _norm(hidden, gain, half, x_norm=None):
    rows, width = hidden.shape
    step = 128
    n = rows // 2 // step

    def kernel(h_ref, g_ref, *refs):
        x_ref, xs_ref = refs[-2:]
        h = h_ref[...].astype(F32)
        inv_rms = lax.rsqrt(jnp.mean(h * h, axis=-1, keepdims=True) + NORM_EPS)
        x = (h * inv_rms * g_ref[...]).astype(BF16)
        x_ref[...] = x
        xs_ref[...] = x.astype(F32)

    at = pl.BlockSpec((step, width), lambda i: (half * n + i, 0))
    return pl.pallas_call(
        kernel,
        grid=(n,),
        out_shape=[jax.ShapeDtypeStruct((rows, width), BF16), jax.ShapeDtypeStruct((rows // 2, width), F32)],
        in_specs=[at, _whole((1, width))] + [_any()] * (x_norm is not None),
        out_specs=[at, pl.BlockSpec((step, width), lambda i: (i, 0))],
        input_output_aliases={2: 0} if x_norm is not None else {},
        compiler_params=_params(),
        cost_estimate=_cost(rows * width * 128, rows * width * 4),
    )(*((hidden, gain) if x_norm is None else (hidden, gain, x_norm)))


def _logits(x, row, count, w, n_tp, n_dp):
    rows, width = x.shape
    vocab = w.shape[1]
    cols = 1024
    steps = vocab // cols

    def kernel(x_ref, row_ref, cnt_ref, cnt_any, w_ref, z_ref, mrow_ref, mcol_ref, m_ref, s_ref, t_ref, lab_ref, st_buf, cnt_buf, cs_sem, cr_sem, ss_sem, sr_sem):
        i = pl.program_id(0)
        tp, dp = lax.axis_index('tp'), lax.axis_index('dp')

        def tell(k):
            return _send(cnt_any, cnt_buf.at[k - 1], cs_sem.at[k - 1], cr_sem.at[k - 1], {'dp': (dp + k) % n_dp})

        def give(k, slot):
            return _send(st_buf.at[slot], st_buf.at[slot], ss_sem.at[k - 1], sr_sem.at[k - 1], {'tp': (tp + k) % n_tp})

        @pl.when(i == 0)
        def _():
            _meet([{'tp': (tp + k) % n_tp} for k in range(1, n_tp)] + [{'dp': (dp + k) % n_dp} for k in range(1, n_dp)])
            for k in range(1, n_dp):
                tell(k).start()
            m_ref[...] = jnp.full_like(m_ref, -jnp.inf)
            s_ref[...] = jnp.zeros_like(s_ref)
            t_ref[...] = jnp.zeros_like(t_ref)
            lab_ref[...] = _columns(row_ref[...])

        z = jnp.dot(x_ref[...], w_ref[...], preferred_element_type=F32)
        z_ref[...] = z
        rel = lab_ref[:, 0:1].astype(jnp.int32) - (tp * vocab + cols * i)
        lane = lax.broadcasted_iota(jnp.int32, (rows, 128), 1)
        old = m_ref[...]
        top = old
        for g in range(cols // 128):
            top = jnp.maximum(top, z[:, g * 128:(g + 1) * 128])
        total = s_ref[...] * jnp.exp(old - top)
        target = t_ref[...]
        for g in range(cols // 128):
            z_g = z[:, g * 128:(g + 1) * 128]
            total = total + jnp.exp(z_g - top)
            target = target + jnp.where(lane == rel - g * 128, z_g, 0.0)
        m_ref[...] = top
        s_ref[...] = total
        t_ref[...] = target

        @pl.when(i == steps - 1)
        def _():
            top, total = m_ref[...], s_ref[...]
            row_max = jnp.max(top, axis=1, keepdims=True)
            row_sum = jnp.sum(total * jnp.exp(top - row_max), axis=1, keepdims=True)
            row_target = jnp.sum(t_ref[...], axis=1, keepdims=True)
            st_buf[tp] = jnp.where(lane == 0, row_max, jnp.where(lane == 1, row_sum, row_target)).T[0:8]
            for k in range(1, n_dp):
                tell(k).wait()
            for k in range(1, n_tp):
                give(k, tp).start()
            n_valid = cnt_ref[0:1, 0:1]
            for k in range(1, n_dp):
                n_valid = n_valid + cnt_buf[k - 1, 0:1, 0:1]
            for k in range(1, n_tp):
                give(k, tp).wait_send()
                give(k, (tp + n_tp - k) % n_tp).wait_recv()
            top = st_buf[0, 0:1]
            for k in range(1, n_tp):
                top = jnp.maximum(top, st_buf[k, 0:1])
            total = st_buf[0, 1:2] * jnp.exp(st_buf[0, 0:1] - top)
            target = st_buf[0, 2:3]
            for k in range(1, n_tp):
                total = total + st_buf[k, 1:2] * jnp.exp(st_buf[k, 0:1] - top)
                target = target + st_buf[k, 2:3]
            lse = top + jnp.log(total)
            valid = row_ref[1:2]
            sub = lax.broadcasted_iota(jnp.int32, (8, rows), 0)
            meta = jnp.where(sub == 0, lse, jnp.where(sub == 1, row_ref[0:1], jnp.where(sub == 2, valid / n_valid, jnp.where(sub == 3, (lse - target) * valid, n_valid))))
            mrow_ref[...] = meta
            mcol_ref[...] = _columns(meta)

    return pl.pallas_call(
        kernel,
        grid=(steps,),
        out_shape=[jax.ShapeDtypeStruct((rows, vocab), F32), jax.ShapeDtypeStruct((8, rows), F32), jax.ShapeDtypeStruct((rows, 128), F32)],
        in_specs=[_whole((rows, width)), _whole((8, rows)), _whole((8, 128)), _any(), pl.BlockSpec((width, cols), lambda i: (0, i))],
        out_specs=[pl.BlockSpec((rows, cols), lambda i: (0, i)), _whole((8, rows)), _whole((rows, 128))],
        scratch_shapes=[pltpu.VMEM((rows, 128), F32)] * 4
        + [pltpu.VMEM((n_tp, 8, rows), F32), pltpu.VMEM((n_dp - 1, 8, 128), F32)]
        + [pltpu.SemaphoreType.DMA((n_dp - 1,))] * 2 + [pltpu.SemaphoreType.DMA((n_tp - 1,))] * 2,
        compiler_params=_params(collective_id=1, has_side_effects=True),
        cost_estimate=_cost(2 * rows * width * vocab, vocab * (2 * width + 4 * rows)),
    )(x, row, count, count, w)


def _d_logits(z, meta, first):
    rel = meta[:, 1:2].astype(jnp.int32) - first
    hit = lax.broadcasted_iota(jnp.int32, z.shape, 1) == rel
    return ((jnp.exp(z - meta[:, 0:1]) - jnp.where(hit, 1.0, 0.0)) * meta[:, 2:3]).astype(BF16)


def _d_norm(z, mcol, mrow, w, n_cp, n_dp):
    rows, vocab = z.shape
    width = w.shape[0]
    cols = 1024
    steps = vocab // cols
    groups = n_cp * n_dp

    def kernel(z_ref, mcol_ref, mrow_any, w_ref, acc_ref, all_ref, buf, own_sem, send_sem, recv_sem):
        i = pl.program_id(0)
        me, device = _plane(n_dp)
        own = pltpu.make_async_copy(mrow_any, buf.at[me], own_sem)

        def give(e, slot):
            return _send(mrow_any, buf.at[slot], send_sem.at[e - 1], recv_sem.at[e - 1], device((me + e) % groups))

        @pl.when(i == 0)
        def _():
            own.start()
            _meet([device((me + e) % groups) for e in range(1, groups)])
            for e in range(1, groups):
                give(e, me).start()
            acc_ref[...] = jnp.zeros_like(acc_ref)

        d = _d_logits(z_ref[...], mcol_ref[...], lax.axis_index('tp') * vocab + i * cols)
        acc_ref[...] += lax.dot_general(d, w_ref[...], (((1,), (1,)), ((), ())), preferred_element_type=F32)

        @pl.when(i == steps - 1)
        def _():
            own.wait()
            for e in range(1, groups):
                give(e, me).wait_send()
                give(e, (me + groups - e) % groups).wait_recv()
            all_ref[...] = buf[...]

    return pl.pallas_call(
        kernel,
        grid=(steps,),
        out_shape=[jax.ShapeDtypeStruct((rows, width), F32), jax.ShapeDtypeStruct((groups, 8, rows), F32)],
        in_specs=[pl.BlockSpec((rows, cols), lambda i: (0, i)), _whole((rows, 128)), _any(), pl.BlockSpec((width, cols), lambda i: (0, i))],
        out_specs=[_whole((rows, width)), _whole((groups, 8, rows))],
        scratch_shapes=[pltpu.VMEM((groups, 8, rows), F32), pltpu.SemaphoreType.DMA] + [pltpu.SemaphoreType.DMA((groups - 1,))] * 2,
        compiler_params=_params(collective_id=2, has_side_effects=True),
        cost_estimate=_cost(2 * rows * width * vocab, vocab * (2 * width + 4 * rows)),
    )(z, mcol, mrow, w)


class _Split:
    def __init__(self, vocab, groups):
        self.vocab, self.groups = vocab, groups
        self.blocks = vocab // COLS
        self.n_f = (self.blocks - groups - 2) // 2
        self.g0 = 2 * self.n_f
        self.r0 = self.g0 + groups
        self.n = 1 + self.n_f

    def block(self, b, me, core):
        return jnp.where(b == 0, self.g0 + me, core * self.n_f + b - 1)


def _part(x_b, meta, w, first):
    rows = jnp.concatenate([meta[k] for k in range(meta.shape[0])], axis=1) if meta.shape[0] > 1 else meta[0]
    d = _d_logits(jnp.dot(x_b, w, preferred_element_type=F32), _columns(rows), first)
    return lax.dot_general(x_b, d, (((0,), (0,)), ((), ())), preferred_element_type=F32)


def _head_a(x, meta, w, d_x_norm, split, n_tp, n_dp):
    rows, width = x.shape
    half = meta.shape[2] // 2
    n_tok = rows // TOK
    sub = d_x_norm.shape[0] // n_tp

    def kernel(x_ref, meta_ref, w_ref, dx_any, acc_ref, got_any, leg, mid, send_sem, recv_sem, leg_sem, mid_sem):
        b, i = pl.program_id(0), pl.program_id(1)
        step = b * n_tok + i
        stage = [split.n * n_tok * part // 32 for part in (10, 12)]
        tp = lax.axis_index('tp')
        me, _ = _plane(n_dp)
        inner = (tp == 1) | (tp == 2)
        far = jnp.where(tp < 2, 3, 0)

        def quarter(q):
            return dx_any.at[pl.ds(pl.multiple_of(q * sub, 8), sub)]

        def give(to, src):
            return _send(src, got_any.at[tp], send_sem.at[to], recv_sem.at[tp], {'tp': to})

        def arrive(frm):
            return _send(mid, got_any.at[frm], send_sem.at[frm], recv_sem.at[frm], {'tp': frm})

        first_leg = _send(quarter(far), leg, leg_sem.at[0], leg_sem.at[1], {'tp': jnp.where(tp == 0, 1, 2)})
        load_mid = pltpu.make_async_copy(quarter(far), mid, mid_sem)

        @pl.when((b == 0) & (i == 0))
        def _():
            _meet([{'tp': (tp + k) % n_tp} for k in range(1, n_tp)])

            @pl.when(inner)
            def _():
                load_mid.start()
                give(3 - tp, quarter(3 - tp)).start()
                give(3 - far, quarter(3 - far)).start()

            @pl.when(jnp.logical_not(inner))
            def _():
                first_leg.start()

        @pl.when((step == stage[0]) & jnp.logical_not(inner))
        def _():
            for gap in (1, 2):
                to = jnp.where(tp == 0, gap, 3 - gap)
                give(to, quarter(to)).start()

        @pl.when((step == stage[1]) & inner)
        def _():
            load_mid.wait()
            first_leg.wait_recv()
            mid[...] += leg[...]

        @pl.when((step == stage[1] + 1) & inner)
        def _():
            give(far, mid).start()

        @pl.when(i == 0)
        def _():
            acc_ref[...] = jnp.zeros_like(acc_ref)

        first = tp * split.vocab + split.block(b, me, lax.axis_index('dp') % 2) * COLS
        acc_ref[...] += _part(x_ref[...].astype(BF16), meta_ref, w_ref[...], first)

        @pl.when((b == split.n - 1) & (i == n_tok - 1))
        def _():
            @pl.when(inner)
            def _():
                for q in range(n_tp):
                    @pl.when(tp != q)
                    def _():
                        give(q, mid).wait_send()
                        arrive(q).wait_recv()

            @pl.when(jnp.logical_not(inner))
            def _():
                first_leg.wait_send()
                for q in (1, 2):
                    give(q, mid).wait_send()
                    arrive(q).wait_recv()

    return pl.pallas_call(
        kernel,
        grid=(split.n, n_tok),
        out_shape=[jax.ShapeDtypeStruct((width, split.n * COLS), F32), jax.ShapeDtypeStruct((n_tp, sub, width), F32)],
        in_specs=[
            pl.BlockSpec((TOK, width), lambda b, i: (i, 0)),
            pl.BlockSpec((TOK // half, 8, half), lambda b, i: (i, 0, 0)),
            pl.BlockSpec((width, COLS), lambda b, i: (0, split.block(b, _plane(n_dp)[0], lax.axis_index('dp') % 2))),
            _any(),
        ],
        out_specs=[pl.BlockSpec((width, COLS), lambda b, i: (0, b)), _any()],
        scratch_shapes=[pltpu.VMEM((sub, width), F32)] * 2 + [pltpu.SemaphoreType.DMA((n_tp,))] * 2 + [pltpu.SemaphoreType.DMA((2,)), pltpu.SemaphoreType.DMA],
        compiler_params=_params(collective_id=3, has_side_effects=True),
        cost_estimate=_cost(4 * rows * width * split.n * COLS, split.n * rows * width * 4),
    )(x, meta, w, d_x_norm)


def _head_g(x_first, x, meta, w, part, split, n_dp):
    rows, width = x.shape
    half = meta.shape[2] // 2

    def kernel(xa_ref, x_ref, meta_ref, w_ref, init_ref, acc_ref, xb_ref):
        @pl.when(pl.program_id(0) == 0)
        def _():
            acc_ref[...] = init_ref[...]

        x_b = x_ref[...].astype(BF16)
        xb_ref[0] = xa_ref[...].astype(BF16)
        xb_ref[1] = x_b
        first = lax.axis_index('tp') * split.vocab + (split.g0 + _plane(n_dp)[0]) * COLS
        acc_ref[...] += _part(x_b, meta_ref, w_ref[...], first)

    tile = pl.BlockSpec((half, width), lambda i: (i, 0))
    return pl.pallas_call(
        kernel,
        grid=(rows // half,),
        out_shape=[jax.ShapeDtypeStruct((width, COLS), F32), jax.ShapeDtypeStruct((2, rows, width), BF16)],
        in_specs=[
            tile,
            tile,
            pl.BlockSpec((1, 8, half), lambda i: (i, 0, 1)),
            pl.BlockSpec((width, COLS), lambda i: (0, split.g0 + _plane(n_dp)[0])),
            _whole((width, COLS)),
        ],
        out_specs=[_whole((width, COLS)), pl.BlockSpec((2, half, width), lambda i: (0, i, 0))],
        compiler_params=_params(),
        cost_estimate=_cost(4 * rows * width * COLS, rows * width * 6),
    )(x_first, x, meta, w, part)


def _head_f(x, meta, w, part, d_hid, d_gain, split, n_tp, n_cp, n_dp):
    _, rows, width = x.shape
    half = meta.shape[2] // 2
    n_f, groups = split.n_f, n_cp * n_dp
    n_tok = rows // TOK
    sub = d_hid.shape[0]

    def kernel(x_ref, meta_ref, w_ref, init_any, dh_any, dg_any, out_any, dhall_any, dg_ref, acc, dg_z, dg_s, dg_x, init_sem, own_sem, send_sem, recv_sem, hs_sem, hr_sem, fs_sem, zs_sem, zr_sem, zo_sem, xs_sem, xr_sem):
        j, i = pl.program_id(0), pl.program_id(1)
        step = j * n_tok + i
        stage = [n_f * n_tok * part // 28 for part in (9, 12, 18, 21)]
        tp, dp = lax.axis_index('tp'), lax.axis_index('dp')
        inner = (tp == 1) | (tp == 2)
        me, device = _plane(n_dp)
        core = dp % 2
        slot = j % 2
        z_peers = [{'tp': (tp + k) % n_tp} for k in range(1, n_tp)]

        def at(owner, jj):
            return out_any.at[:, pl.ds(pl.multiple_of((owner * n_f + jj) * COLS, COLS), COLS)]

        def init(jj):
            return pltpu.make_async_copy(init_any.at[:, pl.ds(pl.multiple_of((jj + 1) * COLS, COLS), COLS)], acc.at[jj % 2], init_sem.at[jj % 2])

        def own(jj):
            return pltpu.make_async_copy(acc.at[jj % 2], at(core, jj), own_sem.at[jj % 2])

        def swap(jj, owner):
            return _send(acc.at[jj % 2], at(owner, jj), send_sem.at[jj % 2], recv_sem.at[jj], {'dp': dp + 1 - 2 * core})

        def hid(to, h):
            rows_h = pl.ds(h * (sub // 2), sub // 2)
            return _send(dh_any.at[rows_h], dhall_any.at[tp, rows_h], hs_sem.at[to, h], hr_sem.at[tp, h], {'tp': to})

        def relay(row, to, h):
            at_h = dhall_any.at[row, pl.ds(h * (sub // 2), sub // 2)]
            return _send(at_h, at_h, fs_sem.at[h], hr_sem.at[row, h], {'tp': to})

        def gain_z(k, row):
            return _send(dg_any, dg_z.at[row], zs_sem.at[k - 1], zr_sem.at[k - 1], z_peers[k - 1])

        def gain_x(e, row):
            return _send(dg_s, dg_x.at[row], xs_sem.at[e - 1], xr_sem.at[e - 1], device((me + e) % groups))

        gain_own = pltpu.make_async_copy(dg_any, dg_z.at[tp], zo_sem)

        def across(h, act):
            getattr(hid(jnp.where(tp < 2, tp + 2, tp - 2), h), act)()

        def beside(inward, act):
            for h in range(2):
                getattr(hid(jnp.where((tp < 2) == inward, tp + 1, tp - 1), h), act)()

        def pass_on(h):
            relay(3 * (2 - tp), 3 * (tp - 1), h).wait_recv()
            relay(3 * (2 - tp), 3 * (tp - 1), h).start()

        @pl.when((j == 0) & (i == 0))
        def _():
            init(0).start()
            gain_own.start()
            _meet(z_peers + [device((me + e) % groups) for e in range(1, groups)])
            for k in range(1, n_tp):
                gain_z(k, tp).start()
            across(0, 'start')

            @pl.when(inner)
            def _():
                beside(False, 'start')

        @pl.when(step == stage[0])
        def _():
            across(1, 'start')

        @pl.when((step == stage[1]) & inner)
        def _():
            pass_on(0)

        @pl.when(step == stage[2])
        def _():
            beside(True, 'start')

        @pl.when((step == stage[3]) & inner)
        def _():
            pass_on(1)

        @pl.when((j == 1) & (i == 0))
        def _():
            gain_own.wait()
            for k in range(1, n_tp):
                gain_z(k, tp).wait_send()
                gain_z(k, (tp + n_tp - k) % n_tp).wait_recv()
            total = dg_z[0]
            for k in range(1, n_tp):
                total = total + dg_z[k]
            dg_s[...] = total
            dg_x[me] = total

        @pl.when((j == 1) & (i == n_tok - 1))
        def _():
            for e in range(1, groups):
                gain_x(e, me).start()

        @pl.when(i == 0)
        def _():
            init(j).wait()

        @pl.when(i == n_tok // 2)
        def _():
            @pl.when(j >= 1)
            def _():
                own(j - 1).wait()
                swap(j - 1, core).wait_send()

            @pl.when(j < n_f - 1)
            def _():
                init(j + 1).start()

        first = tp * split.vocab + (core * n_f + j) * COLS
        acc[slot] += _part(x_ref[0], meta_ref, w_ref[...], first)

        @pl.when(i == n_tok - 1)
        def _():
            own(j).start()
            swap(j, core).start()

        @pl.when((j == n_f - 1) & (i == n_tok - 1))
        def _():
            for e in range(1, groups):
                gain_x(e, me).wait_send()
                gain_x(e, (me + groups - e) % groups).wait_recv()
            total = dg_x[0]
            for e in range(1, groups):
                total = total + dg_x[e]
            dg_ref[...] = total
            own(j).wait()
            swap(j, core).wait_send()
            for jj in range(n_f):
                swap(jj, 1 - core).wait_recv()
            for h in range(2):
                across(h, 'wait_send')
            beside(True, 'wait_send')

            @pl.when(inner)
            def _():
                beside(False, 'wait_send')
                for h in range(2):
                    relay(0, 0, h).wait_send()

            for row in range(n_tp):
                relayed = ((tp == 2) & (row == 0)) | ((tp == 1) & (row == 3))

                @pl.when((row != tp) & jnp.logical_not(relayed))
                def _():
                    for h in range(2):
                        relay(row, tp, h).wait_recv()

    return pl.pallas_call(
        kernel,
        grid=(n_f, n_tok),
        out_shape=[jax.ShapeDtypeStruct((width, 2 * n_f * COLS), F32), jax.ShapeDtypeStruct((n_tp, sub, width), F32), jax.ShapeDtypeStruct((8, width), F32)],
        in_specs=[
            pl.BlockSpec((1, TOK, width), lambda j, i: (1, i, 0)),
            pl.BlockSpec((TOK // half, 8, half), lambda j, i: (i, 0, 1)),
            pl.BlockSpec((width, COLS), lambda j, i: (0, lax.axis_index('dp') % 2 * n_f + j)),
            _any(),
            _any(),
            _any(),
        ],
        out_specs=[_any(), _any(), _whole((8, width))],
        scratch_shapes=[pltpu.VMEM((2, width, COLS), F32), pltpu.VMEM((n_tp, 8, width), F32), pltpu.VMEM((8, width), F32), pltpu.VMEM((groups, 8, width), F32)]
        + [pltpu.SemaphoreType.DMA((2,))] * 3 + [pltpu.SemaphoreType.DMA((n_f,)), pltpu.SemaphoreType.DMA((n_tp, 2)), pltpu.SemaphoreType.DMA((n_tp, 2)), pltpu.SemaphoreType.DMA((2,))]
        + [pltpu.SemaphoreType.DMA((n_tp - 1,))] * 2 + [pltpu.SemaphoreType.DMA] + [pltpu.SemaphoreType.DMA((groups - 1,))] * 2,
        compiler_params=_params(collective_id=4, has_side_effects=True),
        cost_estimate=_cost(4 * rows * width * n_f * COLS, n_f * rows * width * 2),
    )(x, meta, w, part, d_hid, d_gain)


def _head_r(x, meta, w, head_f, head_g, d_hid, d_hid_all, split, n_tp):
    _, rows, width = x.shape
    half = meta.shape[2] // 2
    vocab, groups = split.vocab, split.groups
    steps = 2 * groups
    f_wide, r_wide = split.g0 * COLS, 2 * COLS
    strip = width // steps
    per_q = steps // n_tp
    sub = d_hid.shape[0]
    piece = sub // per_q

    def kernel(x_ref, meta_ref, w_ref, f_any, g_any, dh_ref, dhall_ref, out_any, hid_ref, acc, f_buf, g_buf, own_sem, in_sem, out_sem):
        i = pl.program_id(0)
        own = pltpu.make_async_copy(acc, out_any.at[:, pl.ds(split.r0 * COLS, r_wide)], own_sem)

        def places(s):
            at = pl.ds(pl.multiple_of(s * strip, 8), strip)
            g_from = pl.ds(pl.multiple_of(s * (width // 2), 8), width // 2)
            g_rows = pl.ds(pl.multiple_of(s % 2 * (width // 2), 8), width // 2)
            g_cols = pl.ds(pl.multiple_of((split.g0 + s // 2) * COLS, COLS), COLS)
            return f_any.at[at], out_any.at[at, pl.ds(0, f_wide)], g_any.at[g_from], out_any.at[g_rows, g_cols]

        def load(s):
            f_src, _, g_src, _ = places(s)
            return (pltpu.make_async_copy(f_src, f_buf.at[s % 2], in_sem.at[0, s % 2]),
                    pltpu.make_async_copy(g_src, g_buf.at[s % 2], in_sem.at[1, s % 2]))

        def store(s):
            _, f_dst, _, g_dst = places(s)
            return (pltpu.make_async_copy(f_buf.at[s % 2], f_dst, out_sem.at[0, s % 2]),
                    pltpu.make_async_copy(g_buf.at[s % 2], g_dst, out_sem.at[1, s % 2]))

        def each(copies, act):
            for c in copies:
                getattr(c, act)()

        @pl.when(i == 0)
        def _():
            each(load(0), 'start')
            acc[...] = jnp.zeros_like(acc)

        @pl.when(i >= 1)
        def _():
            each(load(i - 1), 'wait')
            each(store(i - 1), 'start')

            @pl.when(i >= 2)
            def _():
                each(store(i - 2), 'wait')

            each(load(i), 'start')

        hid_ref[...] = jnp.where(i // per_q == lax.axis_index('tp'), dh_ref[...], dhall_ref[0]).astype(BF16)
        acc[...] += _part(x_ref[0], meta_ref, w_ref[...], lax.axis_index('tp') * vocab + split.r0 * COLS)

        @pl.when(i == steps - 1)
        def _():
            own.start()
            each(load(i), 'wait')
            each(store(i), 'start')
            each(store(i - 1), 'wait')
            each(store(i), 'wait')
            own.wait()

    return pl.pallas_call(
        kernel,
        grid=(steps,),
        out_shape=[jax.ShapeDtypeStruct((width, vocab), F32), jax.ShapeDtypeStruct((n_tp * sub, width), BF16)],
        in_specs=[
            pl.BlockSpec((1, half, width), lambda i: (i // groups, i % groups, 0)),
            pl.BlockSpec((1, 8, half), lambda i: (i % groups, 0, i // groups)),
            pl.BlockSpec((width, r_wide), lambda i: (0, split.r0 // 2)),
            _any(),
            _any(),
            pl.BlockSpec((piece, width), lambda i: (i % per_q, 0)),
            pl.BlockSpec((1, piece, width), lambda i: (i // per_q, i % per_q, 0)),
        ],
        out_specs=[_any(), pl.BlockSpec((piece, width), lambda i: (i, 0))],
        scratch_shapes=[pltpu.VMEM((width, r_wide), F32), pltpu.VMEM((2, strip, f_wide), F32), pltpu.VMEM((2, width // 2, COLS), F32)]
        + [pltpu.SemaphoreType.DMA] + [pltpu.SemaphoreType.DMA((2, 2))] * 2,
        compiler_params=_params(),
        cost_estimate=_cost(8 * rows * width * r_wide, width * vocab * 8),
    )(x, meta, w, head_f, head_g, d_hid, d_hid_all)


def _finish(hidden, d_x_norm, got, gain, n_tp):
    rows, width = hidden.shape
    sub = rows // n_tp
    step = 64
    n = sub // step

    def kernel(h_ref, own_ref, got_ref, g_ref, dh_ref, dg_ref):
        @pl.when(pl.program_id(0) == 0)
        def _():
            dg_ref[...] = jnp.zeros_like(dg_ref)

        h = h_ref[...].astype(F32)
        inv_rms = lax.rsqrt(jnp.mean(h * h, axis=-1, keepdims=True) + NORM_EPS)
        x = h * inv_rms
        d = own_ref[...]
        tp = lax.axis_index('tp')
        for q in range(n_tp):
            d = d + jnp.where((q != tp) & (q - tp < 3) & (tp - q < 3), got_ref[q], 0.0)
        dg_ref[0:1] += jnp.sum(d * x, axis=0, keepdims=True)
        d_x = d * g_ref[...]
        dh_ref[...] = (inv_rms * (d_x - x * jnp.mean(d_x * x, axis=-1, keepdims=True))).astype(BF16).astype(F32)

    return pl.pallas_call(
        kernel,
        grid=(n,),
        out_shape=[jax.ShapeDtypeStruct((sub, width), F32), jax.ShapeDtypeStruct((8, width), F32)],
        in_specs=[
            pl.BlockSpec((step, width), lambda i: (lax.axis_index('tp') * n + i, 0)),
            pl.BlockSpec((step, width), lambda i: (lax.axis_index('tp') * n + i, 0)),
            pl.BlockSpec((n_tp, step, width), lambda i: (0, i, 0)),
            _whole((1, width)),
        ],
        out_specs=[pl.BlockSpec((step, width), lambda i: (i, 0)), _whole((8, width))],
        compiler_params=_params(),
        cost_estimate=_cost(sub * width * 256, sub * width * 24),
    )(hidden, d_x_norm, got, gain)


def solution(mesh):
    n_tp, n_cp, n_dp = mesh.shape['tp'], mesh.shape['cp'], mesh.shape['dp']
    groups = n_cp * n_dp

    def part_fn(hidden, tokens, seq_lens, norm_gain, w_head):
        n_seq, local_len, width = hidden.shape
        n_tok = n_seq * local_len
        seg_len = local_len // 2
        split = _Split(w_head.shape[1], groups)
        cp_rank = lax.axis_index('cp')
        gain = norm_gain.reshape(1, width)
        hidden_rows = hidden.reshape(n_tok, width)

        x_norm, send_a = _norm(hidden_rows, gain, 0)
        x_a = lax.all_gather(send_a, ('cp', 'dp'), axis=0, tiled=True)
        x_norm, send_b = _norm(hidden_rows, gain, 1, x_norm)
        x_b = lax.all_gather(send_b, ('cp', 'dp'), axis=0, tiled=True)

        edge = lax.ppermute(jnp.where(cp_rank == 0, tokens[:, seg_len], tokens[:, 0]), 'cp', [(0, 1), (1, 0)])
        first_end = jnp.where(cp_rank == 0, edge, tokens[:, seg_len])
        second_end = jnp.where(cp_rank == 0, 0, edge)
        labels = jnp.concatenate([tokens[:, 1:seg_len], first_end[:, None], tokens[:, seg_len + 1:], second_end[:, None]], axis=1)
        seg_pos = jnp.arange(seg_len)
        positions = jnp.concatenate([cp_rank * seg_len + seg_pos, (2 * n_cp - 1 - cp_rank) * seg_len + seg_pos])
        valid = (positions[None, :] + 1 < seq_lens[:, None]).astype(F32)
        row = jnp.concatenate([labels.astype(F32).reshape(1, n_tok), valid.reshape(1, n_tok), jnp.zeros((6, n_tok), F32)])
        count = jnp.broadcast_to(jnp.sum(seq_lens - 1).astype(F32), (8, 128))

        logits, meta_row, meta_col = _logits(x_norm, row, count, w_head, n_tp, n_dp)
        d_x_norm, meta = _d_norm(logits, meta_col, meta_row, w_head, n_cp, n_dp)
        tok_loss = meta_row[3].reshape(n_seq, local_len)
        loss_mean = jnp.sum(meta[:, 3]) / meta[0, 4, 0]
        meta, tok_loss, loss_mean = lax.optimization_barrier((meta, tok_loss, loss_mean))
        part, got = _head_a(x_a, meta, w_head, d_x_norm, split, n_tp, n_dp)
        d_head_g, x_all = _head_g(x_a, x_b, meta, w_head, part, split, n_dp)
        got, d_head_g = lax.optimization_barrier((got, d_head_g))
        d_head_g = lax.all_gather(d_head_g, ('cp', 'dp'), axis=0, tiled=True)
        d_hid, d_gain = _finish(hidden_rows, d_x_norm, got, gain, n_tp)
        d_head_f, d_hid_all, d_gain = _head_f(x_all, meta, w_head, part, d_hid, d_gain, split, n_tp, n_cp, n_dp)
        d_head, d_hidden = _head_r(x_all, meta, w_head, d_head_f, d_head_g, d_hid, d_hid_all, split, n_tp)

        return tok_loss, loss_mean, d_hidden.reshape(hidden.shape), d_gain[0], d_head

    return jax.shard_map(part_fn, mesh=mesh, in_specs=(P('dp', 'cp', None), P('dp', 'cp'), P('dp'), P(None), P(None, 'tp')), out_specs=(P('dp', 'cp'), P(), P('dp', 'cp', None), P(None), P(None, 'tp')), check_vma=False)
```

```python
import jax
import jax.numpy as jnp
from jax import lax
from jax.sharding import PartitionSpec as P
from jax.experimental import pallas as pl
from jax.experimental.pallas import tpu as pltpu

NORM_EPS = 1e-5
F32, BF16 = jnp.float32, jnp.bfloat16
COLS = 512
TOK = 1024
VMEM = 63_000_000
MESH = pl.DeviceIdType.MESH


def _params(**kw):
    return pltpu.CompilerParams(vmem_limit_bytes=VMEM, **kw)


def _cost(flops, bytes_accessed):
    return pl.CostEstimate(flops=int(flops), bytes_accessed=int(bytes_accessed), transcendentals=0)


def _any():
    return pl.BlockSpec(memory_space=pl.ANY)


def _whole(shape):
    return pl.BlockSpec(shape, lambda *ids: (0,) * len(shape))


def _meet(peers):
    barrier = pltpu.get_barrier_semaphore()
    for peer in peers:
        pl.semaphore_signal(barrier, inc=1, device_id=peer, device_id_type=MESH)
    pl.semaphore_wait(barrier, len(peers))


def _send(src, dst, send_sem, recv_sem, peer):
    return pltpu.make_async_remote_copy(src, dst, send_sem, recv_sem, device_id=peer, device_id_type=MESH)


def _plane(n_dp):
    me = lax.axis_index('cp') * n_dp + lax.axis_index('dp')
    return me, lambda p: {'cp': p // n_dp, 'dp': p % n_dp}


def _columns(rows):
    return jnp.concatenate([rows, jnp.zeros((120, rows.shape[1]), F32)], axis=0).T


def _norm(hidden, gain, half, x_norm=None):
    rows, width = hidden.shape
    step = 128
    n = rows // 2 // step

    def kernel(h_ref, g_ref, *refs):
        x_ref, xs_ref = refs[-2:]
        h = h_ref[...].astype(F32)
        inv_rms = lax.rsqrt(jnp.mean(h * h, axis=-1, keepdims=True) + NORM_EPS)
        x = (h * inv_rms * g_ref[...]).astype(BF16)
        x_ref[...] = x
        xs_ref[...] = x.astype(F32)

    at = pl.BlockSpec((step, width), lambda i: (half * n + i, 0))
    return pl.pallas_call(
        kernel,
        grid=(n,),
        out_shape=[jax.ShapeDtypeStruct((rows, width), BF16), jax.ShapeDtypeStruct((rows // 2, width), F32)],
        in_specs=[at, _whole((1, width))] + [_any()] * (x_norm is not None),
        out_specs=[at, pl.BlockSpec((step, width), lambda i: (i, 0))],
        input_output_aliases={2: 0} if x_norm is not None else {},
        compiler_params=_params(),
        cost_estimate=_cost(rows * width * 128, rows * width * 4),
    )(*((hidden, gain) if x_norm is None else (hidden, gain, x_norm)))


def _logits(x, row, count, w, n_tp, n_dp):
    rows, width = x.shape
    vocab = w.shape[1]
    cols = 1024
    steps = vocab // cols

    def kernel(x_ref, row_ref, cnt_ref, cnt_any, w_ref, z_ref, mrow_ref, mcol_ref, m_ref, s_ref, t_ref, lab_ref, st_buf, cnt_buf, cs_sem, cr_sem, ss_sem, sr_sem):
        i = pl.program_id(0)
        tp, dp = lax.axis_index('tp'), lax.axis_index('dp')

        def tell(k):
            return _send(cnt_any, cnt_buf.at[k - 1], cs_sem.at[k - 1], cr_sem.at[k - 1], {'dp': (dp + k) % n_dp})

        def give(k, slot):
            return _send(st_buf.at[slot], st_buf.at[slot], ss_sem.at[k - 1], sr_sem.at[k - 1], {'tp': (tp + k) % n_tp})

        @pl.when(i == 0)
        def _():
            _meet([{'tp': (tp + k) % n_tp} for k in range(1, n_tp)] + [{'dp': (dp + k) % n_dp} for k in range(1, n_dp)])
            for k in range(1, n_dp):
                tell(k).start()
            m_ref[...] = jnp.full_like(m_ref, -jnp.inf)
            s_ref[...] = jnp.zeros_like(s_ref)
            t_ref[...] = jnp.zeros_like(t_ref)
            lab_ref[...] = _columns(row_ref[...])

        z = jnp.dot(x_ref[...], w_ref[...], preferred_element_type=F32)
        z_ref[...] = z
        rel = lab_ref[:, 0:1].astype(jnp.int32) - (tp * vocab + cols * i)
        lane = lax.broadcasted_iota(jnp.int32, (rows, 128), 1)
        old = m_ref[...]
        top = old
        for g in range(cols // 128):
            top = jnp.maximum(top, z[:, g * 128:(g + 1) * 128])
        total = s_ref[...] * jnp.exp(old - top)
        target = t_ref[...]
        for g in range(cols // 128):
            z_g = z[:, g * 128:(g + 1) * 128]
            total = total + jnp.exp(z_g - top)
            target = target + jnp.where(lane == rel - g * 128, z_g, 0.0)
        m_ref[...] = top
        s_ref[...] = total
        t_ref[...] = target

        @pl.when(i == steps - 1)
        def _():
            top, total = m_ref[...], s_ref[...]
            row_max = jnp.max(top, axis=1, keepdims=True)
            row_sum = jnp.sum(total * jnp.exp(top - row_max), axis=1, keepdims=True)
            row_target = jnp.sum(t_ref[...], axis=1, keepdims=True)
            st_buf[tp] = jnp.where(lane == 0, row_max, jnp.where(lane == 1, row_sum, row_target)).T[0:8]
            for k in range(1, n_dp):
                tell(k).wait()
            for k in range(1, n_tp):
                give(k, tp).start()
            n_valid = cnt_ref[0:1, 0:1]
            for k in range(1, n_dp):
                n_valid = n_valid + cnt_buf[k - 1, 0:1, 0:1]
            for k in range(1, n_tp):
                give(k, tp).wait_send()
                give(k, (tp + n_tp - k) % n_tp).wait_recv()
            top = st_buf[0, 0:1]
            for k in range(1, n_tp):
                top = jnp.maximum(top, st_buf[k, 0:1])
            total = st_buf[0, 1:2] * jnp.exp(st_buf[0, 0:1] - top)
            target = st_buf[0, 2:3]
            for k in range(1, n_tp):
                total = total + st_buf[k, 1:2] * jnp.exp(st_buf[k, 0:1] - top)
                target = target + st_buf[k, 2:3]
            lse = top + jnp.log(total)
            valid = row_ref[1:2]
            sub = lax.broadcasted_iota(jnp.int32, (8, rows), 0)
            meta = jnp.where(sub == 0, lse, jnp.where(sub == 1, row_ref[0:1], jnp.where(sub == 2, valid / n_valid, jnp.where(sub == 3, (lse - target) * valid, n_valid))))
            mrow_ref[...] = meta
            mcol_ref[...] = _columns(meta)

    return pl.pallas_call(
        kernel,
        grid=(steps,),
        out_shape=[jax.ShapeDtypeStruct((rows, vocab), F32), jax.ShapeDtypeStruct((8, rows), F32), jax.ShapeDtypeStruct((rows, 128), F32)],
        in_specs=[_whole((rows, width)), _whole((8, rows)), _whole((8, 128)), _any(), pl.BlockSpec((width, cols), lambda i: (0, i))],
        out_specs=[pl.BlockSpec((rows, cols), lambda i: (0, i)), _whole((8, rows)), _whole((rows, 128))],
        scratch_shapes=[pltpu.VMEM((rows, 128), F32)] * 4
        + [pltpu.VMEM((n_tp, 8, rows), F32), pltpu.VMEM((n_dp - 1, 8, 128), F32)]
        + [pltpu.SemaphoreType.DMA((n_dp - 1,))] * 2 + [pltpu.SemaphoreType.DMA((n_tp - 1,))] * 2,
        compiler_params=_params(collective_id=1, has_side_effects=True),
        cost_estimate=_cost(2 * rows * width * vocab, vocab * (2 * width + 4 * rows)),
    )(x, row, count, count, w)


def _d_logits(z, meta, first):
    rel = meta[:, 1:2].astype(jnp.int32) - first
    hit = lax.broadcasted_iota(jnp.int32, z.shape, 1) == rel
    return ((jnp.exp(z - meta[:, 0:1]) - jnp.where(hit, 1.0, 0.0)) * meta[:, 2:3]).astype(BF16)


def _d_norm(z, mcol, mrow, w, n_cp, n_dp):
    rows, vocab = z.shape
    width = w.shape[0]
    cols = 1024
    steps = vocab // cols
    groups = n_cp * n_dp

    def kernel(z_ref, mcol_ref, mrow_any, w_ref, acc_ref, all_ref, buf, own_sem, send_sem, recv_sem):
        i = pl.program_id(0)
        me, device = _plane(n_dp)
        own = pltpu.make_async_copy(mrow_any, buf.at[me], own_sem)

        def give(e, slot):
            return _send(mrow_any, buf.at[slot], send_sem.at[e - 1], recv_sem.at[e - 1], device((me + e) % groups))

        @pl.when(i == 0)
        def _():
            own.start()
            _meet([device((me + e) % groups) for e in range(1, groups)])
            for e in range(1, groups):
                give(e, me).start()
            acc_ref[...] = jnp.zeros_like(acc_ref)

        d = _d_logits(z_ref[...], mcol_ref[...], lax.axis_index('tp') * vocab + i * cols)
        acc_ref[...] += lax.dot_general(d, w_ref[...], (((1,), (1,)), ((), ())), preferred_element_type=F32)

        @pl.when(i == steps - 1)
        def _():
            own.wait()
            for e in range(1, groups):
                give(e, me).wait_send()
                give(e, (me + groups - e) % groups).wait_recv()
            all_ref[...] = buf[...]

    return pl.pallas_call(
        kernel,
        grid=(steps,),
        out_shape=[jax.ShapeDtypeStruct((rows, width), F32), jax.ShapeDtypeStruct((groups, 8, rows), F32)],
        in_specs=[pl.BlockSpec((rows, cols), lambda i: (0, i)), _whole((rows, 128)), _any(), pl.BlockSpec((width, cols), lambda i: (0, i))],
        out_specs=[_whole((rows, width)), _whole((groups, 8, rows))],
        scratch_shapes=[pltpu.VMEM((groups, 8, rows), F32), pltpu.SemaphoreType.DMA] + [pltpu.SemaphoreType.DMA((groups - 1,))] * 2,
        compiler_params=_params(collective_id=2, has_side_effects=True),
        cost_estimate=_cost(2 * rows * width * vocab, vocab * (2 * width + 4 * rows)),
    )(z, mcol, mrow, w)


class _Split:
    def __init__(self, vocab, groups):
        self.vocab, self.groups = vocab, groups
        self.blocks = vocab // COLS
        self.n_f = (self.blocks - groups - 2) // 2
        self.g0 = 2 * self.n_f
        self.r0 = self.g0 + groups
        self.n = 1 + self.n_f

    def block(self, b, me, core):
        return jnp.where(b == 0, self.g0 + me, core * self.n_f + b - 1)


def _part(x_b, meta, w, first):
    rows = jnp.concatenate([meta[k] for k in range(meta.shape[0])], axis=1) if meta.shape[0] > 1 else meta[0]
    d = _d_logits(jnp.dot(x_b, w, preferred_element_type=F32), _columns(rows), first)
    return lax.dot_general(x_b, d, (((0,), (0,)), ((), ())), preferred_element_type=F32)


def _head_a(x, meta, w, d_x_norm, split, n_tp, n_dp):
    rows, width = x.shape
    half = meta.shape[2] // 2
    n_tok = rows // TOK
    sub = d_x_norm.shape[0] // n_tp

    def kernel(x_ref, meta_ref, w_ref, dx_any, acc_ref, got_any, leg, mid, send_sem, recv_sem, leg_sem, mid_sem):
        b, i = pl.program_id(0), pl.program_id(1)
        step = b * n_tok + i
        stage = [split.n * n_tok * part // 32 for part in (10, 12)]
        tp = lax.axis_index('tp')
        me, _ = _plane(n_dp)
        inner = (tp == 1) | (tp == 2)
        far = jnp.where(tp < 2, 3, 0)

        def quarter(q):
            return dx_any.at[pl.ds(pl.multiple_of(q * sub, 8), sub)]

        def give(to, src):
            return _send(src, got_any.at[tp], send_sem.at[to], recv_sem.at[tp], {'tp': to})

        def arrive(frm):
            return _send(mid, got_any.at[frm], send_sem.at[frm], recv_sem.at[frm], {'tp': frm})

        first_leg = _send(quarter(far), leg, leg_sem.at[0], leg_sem.at[1], {'tp': jnp.where(tp == 0, 1, 2)})
        load_mid = pltpu.make_async_copy(quarter(far), mid, mid_sem)

        @pl.when((b == 0) & (i == 0))
        def _():
            _meet([{'tp': (tp + k) % n_tp} for k in range(1, n_tp)])

            @pl.when(inner)
            def _():
                load_mid.start()
                give(3 - tp, quarter(3 - tp)).start()
                give(3 - far, quarter(3 - far)).start()

            @pl.when(jnp.logical_not(inner))
            def _():
                first_leg.start()

        @pl.when((step == stage[0]) & jnp.logical_not(inner))
        def _():
            for gap in (1, 2):
                to = jnp.where(tp == 0, gap, 3 - gap)
                give(to, quarter(to)).start()

        @pl.when((step == stage[1]) & inner)
        def _():
            load_mid.wait()
            first_leg.wait_recv()
            mid[...] += leg[...]

        @pl.when((step == stage[1] + 1) & inner)
        def _():
            give(far, mid).start()

        @pl.when(i == 0)
        def _():
            acc_ref[...] = jnp.zeros_like(acc_ref)

        first = tp * split.vocab + split.block(b, me, lax.axis_index('dp') % 2) * COLS
        acc_ref[...] += _part(x_ref[...].astype(BF16), meta_ref, w_ref[...], first)

        @pl.when((b == split.n - 1) & (i == n_tok - 1))
        def _():
            @pl.when(inner)
            def _():
                for q in range(n_tp):
                    @pl.when(tp != q)
                    def _():
                        give(q, mid).wait_send()
                        arrive(q).wait_recv()

            @pl.when(jnp.logical_not(inner))
            def _():
                first_leg.wait_send()
                for q in (1, 2):
                    give(q, mid).wait_send()
                    arrive(q).wait_recv()

    return pl.pallas_call(
        kernel,
        grid=(split.n, n_tok),
        out_shape=[jax.ShapeDtypeStruct((width, split.n * COLS), F32), jax.ShapeDtypeStruct((n_tp, sub, width), F32)],
        in_specs=[
            pl.BlockSpec((TOK, width), lambda b, i: (i, 0)),
            pl.BlockSpec((TOK // half, 8, half), lambda b, i: (i, 0, 0)),
            pl.BlockSpec((width, COLS), lambda b, i: (0, split.block(b, _plane(n_dp)[0], lax.axis_index('dp') % 2))),
            _any(),
        ],
        out_specs=[pl.BlockSpec((width, COLS), lambda b, i: (0, b)), _any()],
        scratch_shapes=[pltpu.VMEM((sub, width), F32)] * 2 + [pltpu.SemaphoreType.DMA((n_tp,))] * 2 + [pltpu.SemaphoreType.DMA((2,)), pltpu.SemaphoreType.DMA],
        compiler_params=_params(collective_id=3, has_side_effects=True),
        cost_estimate=_cost(4 * rows * width * split.n * COLS, split.n * rows * width * 4),
    )(x, meta, w, d_x_norm)


def _head_g(x, meta, w, part, split, n_dp):
    rows, width = x.shape
    half = meta.shape[2] // 2

    def kernel(x_ref, meta_ref, w_ref, init_ref, acc_ref, xb_ref):
        @pl.when(pl.program_id(0) == 0)
        def _():
            acc_ref[...] = init_ref[...]

        x_b = x_ref[...].astype(BF16)
        xb_ref[0] = x_b
        first = lax.axis_index('tp') * split.vocab + (split.g0 + _plane(n_dp)[0]) * COLS
        acc_ref[...] += _part(x_b, meta_ref, w_ref[...], first)

    return pl.pallas_call(
        kernel,
        grid=(rows // half,),
        out_shape=[jax.ShapeDtypeStruct((width, COLS), F32), jax.ShapeDtypeStruct((2, rows, width), BF16)],
        in_specs=[
            pl.BlockSpec((half, width), lambda i: (i, 0)),
            pl.BlockSpec((1, 8, half), lambda i: (i, 0, 1)),
            pl.BlockSpec((width, COLS), lambda i: (0, split.g0 + _plane(n_dp)[0])),
            _whole((width, COLS)),
        ],
        out_specs=[_whole((width, COLS)), pl.BlockSpec((1, half, width), lambda i: (1, i, 0))],
        compiler_params=_params(),
        cost_estimate=_cost(4 * rows * width * COLS, rows * width * 6),
    )(x, meta, w, part)


def _head_f(x, x_first, meta, w, part, d_hid, d_gain, split, n_tp, n_cp, n_dp):
    _, rows, width = x.shape
    half = meta.shape[2] // 2
    n_f, groups = split.n_f, n_cp * n_dp
    n_tok = rows // TOK
    sub = d_hid.shape[0]
    cut = TOK // 4

    def turn(j, i):
        return jnp.minimum(j * n_tok + i, rows // cut - 1)

    def kernel(x_ref, xa_ref, meta_ref, w_ref, init_any, dh_any, dg_any, out_any, dhall_any, dg_ref, xo_ref, acc, dg_z, dg_s, dg_x, init_sem, own_sem, send_sem, recv_sem, hs_sem, hr_sem, fs_sem, zs_sem, zr_sem, zo_sem, xs_sem, xr_sem):
        j, i = pl.program_id(0), pl.program_id(1)
        step = j * n_tok + i
        stage = [n_f * n_tok * part // 28 for part in (9, 12, 18, 21)]
        tp, dp = lax.axis_index('tp'), lax.axis_index('dp')
        inner = (tp == 1) | (tp == 2)
        me, device = _plane(n_dp)
        core = dp % 2
        slot = j % 2
        z_peers = [{'tp': (tp + k) % n_tp} for k in range(1, n_tp)]

        def at(owner, jj):
            return out_any.at[:, pl.ds(pl.multiple_of((owner * n_f + jj) * COLS, COLS), COLS)]

        def init(jj):
            return pltpu.make_async_copy(init_any.at[:, pl.ds(pl.multiple_of((jj + 1) * COLS, COLS), COLS)], acc.at[jj % 2], init_sem.at[jj % 2])

        def own(jj):
            return pltpu.make_async_copy(acc.at[jj % 2], at(core, jj), own_sem.at[jj % 2])

        def swap(jj, owner):
            return _send(acc.at[jj % 2], at(owner, jj), send_sem.at[jj % 2], recv_sem.at[jj], {'dp': dp + 1 - 2 * core})

        def hid(to, h):
            rows_h = pl.ds(h * (sub // 2), sub // 2)
            return _send(dh_any.at[rows_h], dhall_any.at[tp, rows_h], hs_sem.at[to, h], hr_sem.at[tp, h], {'tp': to})

        def relay(row, to, h):
            at_h = dhall_any.at[row, pl.ds(h * (sub // 2), sub // 2)]
            return _send(at_h, at_h, fs_sem.at[h], hr_sem.at[row, h], {'tp': to})

        def gain_z(k, row):
            return _send(dg_any, dg_z.at[row], zs_sem.at[k - 1], zr_sem.at[k - 1], z_peers[k - 1])

        def gain_x(e, row):
            return _send(dg_s, dg_x.at[row], xs_sem.at[e - 1], xr_sem.at[e - 1], device((me + e) % groups))

        gain_own = pltpu.make_async_copy(dg_any, dg_z.at[tp], zo_sem)

        def across(h, act):
            getattr(hid(jnp.where(tp < 2, tp + 2, tp - 2), h), act)()

        def beside(inward, act):
            for h in range(2):
                getattr(hid(jnp.where((tp < 2) == inward, tp + 1, tp - 1), h), act)()

        def pass_on(h):
            relay(3 * (2 - tp), 3 * (tp - 1), h).wait_recv()
            relay(3 * (2 - tp), 3 * (tp - 1), h).start()

        @pl.when((j == 0) & (i == 0))
        def _():
            init(0).start()
            gain_own.start()
            _meet(z_peers + [device((me + e) % groups) for e in range(1, groups)])
            for k in range(1, n_tp):
                gain_z(k, tp).start()
            across(0, 'start')

            @pl.when(inner)
            def _():
                beside(False, 'start')

        @pl.when(step == stage[0])
        def _():
            across(1, 'start')

        @pl.when((step == stage[1]) & inner)
        def _():
            pass_on(0)

        @pl.when(step == stage[2])
        def _():
            beside(True, 'start')

        @pl.when((step == stage[3]) & inner)
        def _():
            pass_on(1)

        @pl.when((j == 1) & (i == 0))
        def _():
            gain_own.wait()
            for k in range(1, n_tp):
                gain_z(k, tp).wait_send()
                gain_z(k, (tp + n_tp - k) % n_tp).wait_recv()
            total = dg_z[0]
            for k in range(1, n_tp):
                total = total + dg_z[k]
            dg_s[...] = total
            dg_x[me] = total

        @pl.when((j == 1) & (i == n_tok - 1))
        def _():
            for e in range(1, groups):
                gain_x(e, me).start()

        @pl.when(i == 0)
        def _():
            init(j).wait()

        @pl.when(i == n_tok // 2)
        def _():
            @pl.when(j >= 1)
            def _():
                own(j - 1).wait()
                swap(j - 1, core).wait_send()

            @pl.when(j < n_f - 1)
            def _():
                init(j + 1).start()

        xo_ref[0] = xa_ref[...].astype(BF16)
        first = tp * split.vocab + (core * n_f + j) * COLS
        acc[slot] += _part(x_ref[0], meta_ref, w_ref[...], first)

        @pl.when(i == n_tok - 1)
        def _():
            own(j).start()
            swap(j, core).start()

        @pl.when((j == n_f - 1) & (i == n_tok - 1))
        def _():
            for e in range(1, groups):
                gain_x(e, me).wait_send()
                gain_x(e, (me + groups - e) % groups).wait_recv()
            total = dg_x[0]
            for e in range(1, groups):
                total = total + dg_x[e]
            dg_ref[...] = total
            own(j).wait()
            swap(j, core).wait_send()
            for jj in range(n_f):
                swap(jj, 1 - core).wait_recv()
            for h in range(2):
                across(h, 'wait_send')
            beside(True, 'wait_send')

            @pl.when(inner)
            def _():
                beside(False, 'wait_send')
                for h in range(2):
                    relay(0, 0, h).wait_send()

            for row in range(n_tp):
                relayed = ((tp == 2) & (row == 0)) | ((tp == 1) & (row == 3))

                @pl.when((row != tp) & jnp.logical_not(relayed))
                def _():
                    for h in range(2):
                        relay(row, tp, h).wait_recv()

    return pl.pallas_call(
        kernel,
        grid=(n_f, n_tok),
        out_shape=[jax.ShapeDtypeStruct((width, 2 * n_f * COLS), F32), jax.ShapeDtypeStruct((n_tp, sub, width), F32), jax.ShapeDtypeStruct((8, width), F32), jax.ShapeDtypeStruct(x.shape, BF16)],
        in_specs=[
            pl.BlockSpec((1, TOK, width), lambda j, i: (1, i, 0)),
            pl.BlockSpec((cut, width), lambda j, i: (turn(j, i), 0)),
            pl.BlockSpec((TOK // half, 8, half), lambda j, i: (i, 0, 1)),
            pl.BlockSpec((width, COLS), lambda j, i: (0, lax.axis_index('dp') % 2 * n_f + j)),
            _any(),
            _any(),
            _any(),
        ],
        out_specs=[_any(), _any(), _whole((8, width)), pl.BlockSpec((1, cut, width), lambda j, i: (0, turn(j, i), 0))],
        input_output_aliases={0: 3},
        scratch_shapes=[pltpu.VMEM((2, width, COLS), F32), pltpu.VMEM((n_tp, 8, width), F32), pltpu.VMEM((8, width), F32), pltpu.VMEM((groups, 8, width), F32)]
        + [pltpu.SemaphoreType.DMA((2,))] * 3 + [pltpu.SemaphoreType.DMA((n_f,)), pltpu.SemaphoreType.DMA((n_tp, 2)), pltpu.SemaphoreType.DMA((n_tp, 2)), pltpu.SemaphoreType.DMA((2,))]
        + [pltpu.SemaphoreType.DMA((n_tp - 1,))] * 2 + [pltpu.SemaphoreType.DMA] + [pltpu.SemaphoreType.DMA((groups - 1,))] * 2,
        compiler_params=_params(collective_id=4, has_side_effects=True),
        cost_estimate=_cost(4 * rows * width * n_f * COLS, n_f * rows * width * 2),
    )(x, x_first, meta, w, part, d_hid, d_gain)


def _head_r(x, meta, w, head_f, head_g, d_hid, d_hid_all, split, n_tp):
    _, rows, width = x.shape
    half = meta.shape[2] // 2
    vocab, groups = split.vocab, split.groups
    steps = 2 * groups
    f_wide, r_wide = split.g0 * COLS, 2 * COLS
    strip = width // steps
    per_q = steps // n_tp
    sub = d_hid.shape[0]
    piece = sub // per_q

    def kernel(x_ref, meta_ref, w_ref, f_any, g_any, dh_ref, dhall_ref, out_any, hid_ref, acc, f_buf, g_buf, own_sem, in_sem, out_sem):
        i = pl.program_id(0)
        own = pltpu.make_async_copy(acc, out_any.at[:, pl.ds(split.r0 * COLS, r_wide)], own_sem)

        def places(s):
            at = pl.ds(pl.multiple_of(s * strip, 8), strip)
            g_from = pl.ds(pl.multiple_of(s * (width // 2), 8), width // 2)
            g_rows = pl.ds(pl.multiple_of(s % 2 * (width // 2), 8), width // 2)
            g_cols = pl.ds(pl.multiple_of((split.g0 + s // 2) * COLS, COLS), COLS)
            return f_any.at[at], out_any.at[at, pl.ds(0, f_wide)], g_any.at[g_from], out_any.at[g_rows, g_cols]

        def load(s):
            f_src, _, g_src, _ = places(s)
            return (pltpu.make_async_copy(f_src, f_buf.at[s % 2], in_sem.at[0, s % 2]),
                    pltpu.make_async_copy(g_src, g_buf.at[s % 2], in_sem.at[1, s % 2]))

        def store(s):
            _, f_dst, _, g_dst = places(s)
            return (pltpu.make_async_copy(f_buf.at[s % 2], f_dst, out_sem.at[0, s % 2]),
                    pltpu.make_async_copy(g_buf.at[s % 2], g_dst, out_sem.at[1, s % 2]))

        def each(copies, act):
            for c in copies:
                getattr(c, act)()

        @pl.when(i == 0)
        def _():
            each(load(0), 'start')
            acc[...] = jnp.zeros_like(acc)

        @pl.when(i >= 1)
        def _():
            each(load(i - 1), 'wait')
            each(store(i - 1), 'start')

            @pl.when(i >= 2)
            def _():
                each(store(i - 2), 'wait')

            each(load(i), 'start')

        hid_ref[...] = jnp.where(i // per_q == lax.axis_index('tp'), dh_ref[...], dhall_ref[0]).astype(BF16)
        acc[...] += _part(x_ref[0], meta_ref, w_ref[...], lax.axis_index('tp') * vocab + split.r0 * COLS)

        @pl.when(i == steps - 1)
        def _():
            own.start()
            each(load(i), 'wait')
            each(store(i), 'start')
            each(store(i - 1), 'wait')
            each(store(i), 'wait')
            own.wait()

    return pl.pallas_call(
        kernel,
        grid=(steps,),
        out_shape=[jax.ShapeDtypeStruct((width, vocab), F32), jax.ShapeDtypeStruct((n_tp * sub, width), BF16)],
        in_specs=[
            pl.BlockSpec((1, half, width), lambda i: (i // groups, i % groups, 0)),
            pl.BlockSpec((1, 8, half), lambda i: (i % groups, 0, i // groups)),
            pl.BlockSpec((width, r_wide), lambda i: (0, split.r0 // 2)),
            _any(),
            _any(),
            pl.BlockSpec((piece, width), lambda i: (i % per_q, 0)),
            pl.BlockSpec((1, piece, width), lambda i: (i // per_q, i % per_q, 0)),
        ],
        out_specs=[_any(), pl.BlockSpec((piece, width), lambda i: (i, 0))],
        scratch_shapes=[pltpu.VMEM((width, r_wide), F32), pltpu.VMEM((2, strip, f_wide), F32), pltpu.VMEM((2, width // 2, COLS), F32)]
        + [pltpu.SemaphoreType.DMA] + [pltpu.SemaphoreType.DMA((2, 2))] * 2,
        compiler_params=_params(),
        cost_estimate=_cost(8 * rows * width * r_wide, width * vocab * 8),
    )(x, meta, w, head_f, head_g, d_hid, d_hid_all)


def _finish(hidden, d_x_norm, got, gain, n_tp):
    rows, width = hidden.shape
    sub = rows // n_tp
    step = 64
    n = sub // step

    def kernel(h_ref, own_ref, got_ref, g_ref, dh_ref, dg_ref):
        @pl.when(pl.program_id(0) == 0)
        def _():
            dg_ref[...] = jnp.zeros_like(dg_ref)

        h = h_ref[...].astype(F32)
        inv_rms = lax.rsqrt(jnp.mean(h * h, axis=-1, keepdims=True) + NORM_EPS)
        x = h * inv_rms
        d = own_ref[...]
        tp = lax.axis_index('tp')
        for q in range(n_tp):
            d = d + jnp.where((q != tp) & (q - tp < 3) & (tp - q < 3), got_ref[q], 0.0)
        dg_ref[0:1] += jnp.sum(d * x, axis=0, keepdims=True)
        d_x = d * g_ref[...]
        dh_ref[...] = (inv_rms * (d_x - x * jnp.mean(d_x * x, axis=-1, keepdims=True))).astype(BF16).astype(F32)

    return pl.pallas_call(
        kernel,
        grid=(n,),
        out_shape=[jax.ShapeDtypeStruct((sub, width), F32), jax.ShapeDtypeStruct((8, width), F32)],
        in_specs=[
            pl.BlockSpec((step, width), lambda i: (lax.axis_index('tp') * n + i, 0)),
            pl.BlockSpec((step, width), lambda i: (lax.axis_index('tp') * n + i, 0)),
            pl.BlockSpec((n_tp, step, width), lambda i: (0, i, 0)),
            _whole((1, width)),
        ],
        out_specs=[pl.BlockSpec((step, width), lambda i: (i, 0)), _whole((8, width))],
        compiler_params=_params(),
        cost_estimate=_cost(sub * width * 256, sub * width * 24),
    )(hidden, d_x_norm, got, gain)


def solution(mesh):
    n_tp, n_cp, n_dp = mesh.shape['tp'], mesh.shape['cp'], mesh.shape['dp']
    groups = n_cp * n_dp

    def part_fn(hidden, tokens, seq_lens, norm_gain, w_head):
        n_seq, local_len, width = hidden.shape
        n_tok = n_seq * local_len
        seg_len = local_len // 2
        split = _Split(w_head.shape[1], groups)
        cp_rank = lax.axis_index('cp')
        gain = norm_gain.reshape(1, width)
        hidden_rows = hidden.reshape(n_tok, width)

        x_norm, send_a = _norm(hidden_rows, gain, 0)
        x_a = lax.all_gather(send_a, ('cp', 'dp'), axis=0, tiled=True)
        x_norm, send_b = _norm(hidden_rows, gain, 1, x_norm)
        x_b = lax.all_gather(send_b, ('cp', 'dp'), axis=0, tiled=True)

        edge = lax.ppermute(jnp.where(cp_rank == 0, tokens[:, seg_len], tokens[:, 0]), 'cp', [(0, 1), (1, 0)])
        first_end = jnp.where(cp_rank == 0, edge, tokens[:, seg_len])
        second_end = jnp.where(cp_rank == 0, 0, edge)
        labels = jnp.concatenate([tokens[:, 1:seg_len], first_end[:, None], tokens[:, seg_len + 1:], second_end[:, None]], axis=1)
        seg_pos = jnp.arange(seg_len)
        positions = jnp.concatenate([cp_rank * seg_len + seg_pos, (2 * n_cp - 1 - cp_rank) * seg_len + seg_pos])
        valid = (positions[None, :] + 1 < seq_lens[:, None]).astype(F32)
        row = jnp.concatenate([labels.astype(F32).reshape(1, n_tok), valid.reshape(1, n_tok), jnp.zeros((6, n_tok), F32)])
        count = jnp.broadcast_to(jnp.sum(seq_lens - 1).astype(F32), (8, 128))

        logits, meta_row, meta_col = _logits(x_norm, row, count, w_head, n_tp, n_dp)
        d_x_norm, meta = _d_norm(logits, meta_col, meta_row, w_head, n_cp, n_dp)
        tok_loss = meta_row[3].reshape(n_seq, local_len)
        loss_mean = jnp.sum(meta[:, 3]) / meta[0, 4, 0]
        meta, tok_loss, loss_mean = lax.optimization_barrier((meta, tok_loss, loss_mean))
        part, got = _head_a(x_a, meta, w_head, d_x_norm, split, n_tp, n_dp)
        d_head_g, x_all = _head_g(x_b, meta, w_head, part, split, n_dp)
        got, d_head_g = lax.optimization_barrier((got, d_head_g))
        d_head_g = lax.all_gather(d_head_g, ('cp', 'dp'), axis=0, tiled=True)
        d_hid, d_gain = _finish(hidden_rows, d_x_norm, got, gain, n_tp)
        d_head_f, d_hid_all, d_gain, x_all = _head_f(x_all, x_a, meta, w_head, part, d_hid, d_gain, split, n_tp, n_cp, n_dp)
        d_head, d_hidden = _head_r(x_all, meta, w_head, d_head_f, d_head_g, d_hid, d_hid_all, split, n_tp)

        return tok_loss, loss_mean, d_hidden.reshape(hidden.shape), d_gain[0], d_head

    return jax.shard_map(part_fn, mesh=mesh, in_specs=(P('dp', 'cp', None), P('dp', 'cp'), P('dp'), P(None), P(None, 'tp')), out_specs=(P('dp', 'cp'), P(), P('dp', 'cp', None), P(None), P(None, 'tp')), check_vma=False)
```
